256 devices in a mesh: rows: 32 (over z, y), chan: 8 (over x, core).
Axes of the slice: x: 4, y: 4, z: 8, core: 2. Of those that a mesh axis runs over, the one named last changes fastest.
Arguments:
- tokens: float32 [64, 768, 512], P('rows', 'chan'), may hold values from -6 to 6
- spectral: float32 [2, 64, 768, 128], P(None, None, 'chan'), may hold values from -6 to 6
- gain_in: float32 [2, 768], P(None, 'chan'), may hold values from 0.25 to 1.75
- gain_mid: float32 [2, 768], P(None, 'chan'), may hold values from 0.25 to 1.75
- expand: bfloat16 [2, 768, 3072], P(None, 'rows', 'chan'), may hold values from -0.21875 to 0.21875
- expand_bias: bfloat16 [2, 3072], P(None, 'chan'), may hold values from -3 to 3
- shrink: bfloat16 [2, 3072, 768], P(None, 'chan', 'rows'), may hold values from -0.21875 to 0.21875
Outputs:
- result: float32 [64, 768, 512], P('rows', 'chan')
The draws below stay inside these ranges and needn't reach their ends.
All inputs are finite; a program needn't handle non-finite values.
Results may differ from the reference program's by a relative error of at most 0.017.
Values may be sent and summed in bfloat16 or wider, within the bound.
A program may use at most 64 MiB of HBM per device.

```python
import math
import jax
import jax.numpy as jnp
from jax import lax

D = 768
HID = 3072
GRID = 64
LAYERS = 2
BATCH = 8
N_CHAN = 8


def raised(result, rng, source, target, parts, factor):
    owner, partner = [(jnp.arange(result.shape[axis_at]) // (result.shape[axis_at] // parts)).reshape([-1 if axis == axis_at else 1 for axis in range(result.ndim)]) for axis_at in (source, target)]
    chosen = jax.random.permutation(rng, parts)[partner]
    strong = (owner == chosen) | (owner == (partner + parts // 2) % parts)
    return jnp.where(strong, factor * result, result)


def block_levels(stream_key, extent, split, least, top_value):
    def one(position, parts):
        heights = jax.random.uniform(jax.random.fold_in(jax.random.fold_in(stream_key, 6), position), (parts,), jnp.float32, least / len(split), top_value / len(split))
        return jnp.repeat(jnp.exp(heights), extent[position] // parts).reshape((-1,) + (1,) * (len(extent) - position - 1))

    factor_of = one(*split[0])
    for cut in split[1:]:
        factor_of = factor_of * one(*cut)
    return factor_of


def noise(key, shape, spread, limit, pieces=(), kind=jnp.bfloat16):
    drawn = spread * jax.random.normal(key, shape, jnp.float32)
    if pieces:
        drawn = drawn * block_levels(key, shape, pieces, -0.22, 0.18)
    return jnp.clip(drawn, -limit, limit).astype(kind)


def gaussian_with(stream_key, extent, spread, bound, split, heavy, kind=jnp.bfloat16):
    result = spread * jax.random.normal(stream_key, extent, jnp.float32)
    if split:
        result = result * block_levels(stream_key, extent, split, -0.22, 0.18)
    return jnp.clip(raised(result, jax.random.fold_in(stream_key, 3), *heavy), -bound, bound).astype(kind)


def setup_inputs(seed: int = 0) -> dict:
    splits = jax.random.split(jax.random.key(seed), 8)
    return {
        "tokens": noise(splits[0], (GRID, D, BATCH * GRID), 1.0, 6.0, ((0, 32), (1, 8)), jnp.float32),
        "spectral": noise(splits[1], (LAYERS, GRID, D, 2 * GRID), 1.0, 6.0, ((2, 8),), jnp.float32),
        "gain_in": jnp.clip(1.0 + 0.15 * jax.random.normal(splits[2], (LAYERS, D), jnp.float32), 0.25, 1.75),
        "gain_mid": jnp.clip(1.0 + 0.15 * jax.random.normal(splits[3], (LAYERS, D), jnp.float32), 0.25, 1.75),
        "expand": noise(splits[4], (LAYERS, D, HID), D ** -0.5, 0.21875, ((1, 32), (2, 8))),
        "expand_bias": noise(splits[5], (LAYERS, HID), 0.5, 3.0, ((1, 8),)),
        "shrink": gaussian_with(splits[6], (LAYERS, HID, D), HID ** -0.5, 0.21875, ((1, 8), (2, 32)), (1, 2, 32, 2.75)),
    }


def tables(count):
    index = jnp.arange(count, dtype=jnp.int32)
    product = index[:, None] * index[None, :] % count
    angle = product.astype(jnp.float32) * (2.0 * math.pi / count)
    return (jnp.cos(angle), jnp.sin(angle))

def layer_norm(values, gain):
    mean = lax.optimization_barrier(jnp.mean(values, axis=-1, keepdims=True))
    var = lax.optimization_barrier(jnp.mean(values * values, axis=-1, keepdims=True)) - mean * mean
    return (values - mean) * lax.rsqrt(var + 1e-06) * gain

def reference(tokens, spectral, gain_in, gain_mid, expand, expand_bias, shrink):
    highest = lax.Precision.HIGHEST
    cosine, sine = tables(GRID)
    state = tokens.reshape(GRID, D, BATCH, GRID).transpose(2, 0, 3, 1)
    groups = N_CHAN
    width = HID // groups
    for layer in range(LAYERS):
        normed = layer_norm(state, gain_in[layer])
        a_re = jnp.einsum('bhwc,wk->bhkc', normed, cosine, precision=highest)
        a_im = -jnp.einsum('bhwc,wk->bhkc', normed, sine, precision=highest)
        b_re = jnp.einsum('bhkc,hj->bjkc', a_re, cosine, precision=highest) + jnp.einsum('bhkc,hj->bjkc', a_im, sine, precision=highest)
        b_im = jnp.einsum('bhkc,hj->bjkc', a_im, cosine, precision=highest) - jnp.einsum('bhkc,hj->bjkc', a_re, sine, precision=highest)
        filt = spectral[layer].reshape(GRID, D, 2, GRID)
        f_re = filt[:, :, 0, :].transpose(2, 0, 1)
        f_im = filt[:, :, 1, :].transpose(2, 0, 1)
        c_re = b_re * f_re - b_im * f_im
        c_im = b_re * f_im + b_im * f_re
        d_re = jnp.einsum('bjkc,jh->bhkc', c_re, cosine, precision=highest) - jnp.einsum('bjkc,jh->bhkc', c_im, sine, precision=highest)
        d_im = jnp.einsum('bjkc,jh->bhkc', c_im, cosine, precision=highest) + jnp.einsum('bjkc,jh->bhkc', c_re, sine, precision=highest)
        mixed = (jnp.einsum('bhkc,kw->bhwc', d_re, cosine, precision=highest) - jnp.einsum('bhkc,kw->bhwc', d_im, sine, precision=highest)) * (1.0 / (GRID * GRID))
        normed2 = layer_norm(mixed, gain_mid[layer]).astype(jnp.bfloat16).reshape(-1, D)
        pre = jnp.dot(normed2, expand[layer], preferred_element_type=jnp.float32) + expand_bias[layer].astype(jnp.float32)
        hidden = jax.nn.gelu(pre, approximate=True).astype(jnp.bfloat16)
        total = jnp.zeros((hidden.shape[0], D), jnp.float32)
        for group in range(groups):
            part = jnp.dot(hidden[:, group * width:(group + 1) * width], shrink[layer, group * width:(group + 1) * width], preferred_element_type=jnp.float32)
            rounded = lax.optimization_barrier(part.astype(jnp.bfloat16))
            total = total + rounded.astype(jnp.float32)
        branch = total.astype(jnp.bfloat16)
        state = state + branch.astype(jnp.float32).reshape(state.shape)
    return state.transpose(1, 3, 0, 2).reshape(GRID, D, BATCH * GRID)
```

```python
import functools

import jax
import jax.numpy as jnp
import numpy as np
from jax import lax
from jax.experimental import pallas as pl
from jax.experimental.pallas import tpu as pltpu
from jax.sharding import PartitionSpec as P

MESH = pl.DeviceIdType.MESH
F32 = jnp.float32
BF16 = jnp.bfloat16

GRID = 64
LAYERS = 2
NR = 32
NC = 8
NZ, NY = 8, 4
CH = 96
OWN = 3
HID = 384
TAP = 24
PIX = 512
HALF = 256
EPS = 1e-06


def matrices():
    index = np.arange(GRID)
    angle = 2.0 * np.pi * ((index[:, None] * index[None, :]) % GRID) / GRID
    cosine, sine = np.cos(angle), np.sin(angle)
    pairs = np.eye(4)

    def first(table):
        return np.einsum("jh,pq->pjhq", table, pairs).reshape(HALF, HALF)

    def second(table):
        return np.kron(np.eye(2), table)

    forward_rows = np.concatenate([first(cosine), -first(sine)], axis=0)
    forward_lanes = np.block([[second(cosine), -second(sine)], [second(sine), second(cosine)]])
    inverse_lanes = np.block([[second(cosine), second(sine)], [-second(sine), second(cosine)]])
    inverse_rows = np.concatenate([first(cosine).T, -first(sine).T], axis=1)
    spread = np.zeros((HALF, HALF))
    for place in range(8):
        for c in range(32):
            spread[c * 8 + place, place * 32 + c] = 1.0
    return tuple(
        np.asarray(m, dtype=jnp.bfloat16)
        for m in (forward_rows, forward_lanes, inverse_lanes, inverse_rows, spread, spread.T)
    )


def dot(a, b):
    return jnp.dot(a, b, preferred_element_type=F32)


def arrived(ref, sem):
    pltpu.make_async_copy(ref, ref, sem).wait()


def kernel(
    tokens,
    spectral,
    gain_in,
    gain_mid,
    expand,
    bias,
    shrink,
    fwd_rows,
    fwd_lanes,
    inv_lanes,
    inv_rows,
    spread,
    gather,
    out,
    spec_buf,
    filt,
    small_rx,
    stats_rx,
    there_tx,
    there_rx,
    back_tx,
    back_rx,
    ag_tx,
    ag_rx,
    rs_tx,
    rs_rx,
    w_all,
    et,
    st,
    gcol,
    bcol,
    turn,
    spec_sem,
    small_s,
    small_r,
    stats_s,
    stats_r,
    there_s,
    there_r,
    back_s,
    back_r,
    ag_s,
    ag_r,
    rs_s,
    rs_r,
    wy_s,
    wy_r,
    wz_s,
    wz_r,
    wc_s,
    wc_r,
):
    r = lax.axis_index("rows")
    c = lax.axis_index("chan")
    z, y = r // NY, r % NY
    x, core = c // 2, c % 2

    barrier = pltpu.get_barrier_semaphore()

    def greet_row(t, carry):
        pl.semaphore_signal(barrier, inc=1, device_id=((r + t) % NR, c), device_id_type=MESH)
        return carry

    def greet_chan(t, carry):
        pl.semaphore_signal(barrier, inc=1, device_id=(r, (c + t) % NC), device_id_type=MESH)
        return carry

    lax.fori_loop(1, NC, greet_chan, 0)
    lax.fori_loop(1, NR, greet_row, 0)

    group = r // 8 * 8
    lane = r % 8

    def spec_copy(layer, i):
        start = pl.multiple_of(i * NR + group, 8)
        return pltpu.make_async_copy(
            spectral.at[layer, :, pl.ds(start, 8), :], spec_buf.at[layer, i], spec_sem.at[layer, i]
        )

    for layer in range(LAYERS):
        for i in range(OWN):
            spec_copy(layer, i).start()

    eye_tap = (
        lax.broadcasted_iota(jnp.int32, (TAP, TAP), 0)
        == lax.broadcasted_iota(jnp.int32, (TAP, TAP), 1)
    ).astype(F32).astype(BF16)
    for layer in range(LAYERS):
        w_all[layer, core, z, y, 0:3] = expand[layer].reshape(3, 8, HID)
        turned = lax.dot_general(
            eye_tap, shrink[layer], (((1,), (1,)), ((), ())), preferred_element_type=F32
        )
        w_all[layer, core, z, y, 3:6] = turned.astype(BF16).reshape(3, 8, HID)

    small_rx[c] = jnp.zeros((4, PIX), F32)
    turn[...] = jnp.zeros((128, 128), F32)
    small_rx[c, 0:2, 0:CH] = gain_mid[...]
    small_rx[c, 2:4, 0:HID] = bias[...].astype(F32)

    out[...] = tokens[...]

    def put_stats(layer):
        for hl in range(2):
            value = out[hl]
            stats_rx[layer, c, hl : hl + 1, :] = jnp.sum(value, axis=0, keepdims=True)
            stats_rx[layer, c, hl + 2 : hl + 3, :] = jnp.sum(value * value, axis=0, keepdims=True)

    def chan_copy(t, buf, send, recv):
        return pltpu.make_async_remote_copy(
            src_ref=buf.at[c],
            dst_ref=buf.at[c],
            send_sem=send,
            recv_sem=recv,
            device_id=(r, (c + t) % NC),
            device_id_type=MESH,
        )

    def send_all(buf, send, recv):
        def one(t, carry):
            chan_copy(t, buf, send, recv).start()
            return carry

        lax.fori_loop(1, NC, one, 0)

    put_stats(0)
    pl.semaphore_wait(barrier, NR - 1 + NC - 1)
    send_all(stats_rx.at[0], stats_s.at[0], stats_r.at[0])
    send_all(small_rx, small_s, small_r)

    def wy_copy(layer, t):
        ref = w_all.at[layer, core, z, y]
        return pltpu.make_async_remote_copy(
            src_ref=ref,
            dst_ref=ref,
            send_sem=wy_s.at[layer, t],
            recv_sem=wy_r.at[layer, t],
            device_id=(z * NY + (y + t) % NY, c),
            device_id_type=MESH,
        )

    def wz_ref(layer, step, way, mine):
        if mine:
            shift = step - 1
        else:
            shift = step
        at = (z + 2 * NZ - shift) % NZ if way == 0 else (z + shift) % NZ
        ref = w_all.at[layer, core, at]
        if step == 4:
            ref = ref.at[pl.ds(2 * way, 2)]
        return ref

    def wz_copy(layer, step, way):
        ref = wz_ref(layer, step, way, True)
        target = (z + 1) % NZ if way == 0 else (z + NZ - 1) % NZ
        return pltpu.make_async_remote_copy(
            src_ref=ref,
            dst_ref=ref,
            send_sem=wz_s.at[layer, step - 1, way],
            recv_sem=wz_r.at[layer, step - 1, way],
            device_id=(target * NY + y, c),
            device_id_type=MESH,
        )

    def wz_start(layer, step):
        for way in range(2):
            wz_copy(layer, step, way).start()

    def wz_wait(layer, step):
        for way in range(2):
            arrived(wz_ref(layer, step, way, False), wz_r.at[layer, step - 1, way])

    def wc_copy(layer):
        ref = w_all.at[layer, core]
        return pltpu.make_async_remote_copy(
            src_ref=ref,
            dst_ref=ref,
            send_sem=wc_s.at[layer],
            recv_sem=wc_r.at[layer],
            device_id=(r, x * 2 + 1 - core),
            device_id_type=MESH,
        )

    def wy_wait(layer):
        for t in range(1, NY):
            arrived(w_all.at[layer, core, z, (y + NY - t) % NY], wy_r.at[layer, t])

    for layer in range(LAYERS):
        for t in range(1, NY):
            wy_copy(layer, t).start()

    lanes = lax.broadcasted_iota(jnp.int32, (1, CH), 1)
    for layer in range(LAYERS):
        for i in range(OWN):
            spec_copy(layer, i).wait()
            values = spec_buf.at[layer, i].reshape(GRID * 8, 128)[pl.ds(lane, GRID, stride=8), :]
            gain = jnp.sum(
                jnp.where(lanes == i * NR + r, gain_in[layer : layer + 1, :], 0.0), axis=1, keepdims=True
            ) * (1.0 / (GRID * GRID))
            values = values * gain
            filt[layer, i] = jnp.concatenate([values, values], axis=0).T

    def exchange(tx, rx, send, recv):
        def one(t, carry):
            to = (r + t) % NR
            pltpu.make_async_remote_copy(
                src_ref=tx.at[to],
                dst_ref=rx.at[r],
                send_sem=send,
                recv_sem=recv,
                device_id=(to, c),
                device_id_type=MESH,
            ).start()
            return carry

        lax.fori_loop(1, NR, one, 0)
        pltpu.make_async_copy(tx.at[r], rx.at[r], recv).start()

    def as_matrix(rx):
        return jnp.concatenate(
            [rx[:, i].astype(F32).reshape(HALF, 128) for i in range(OWN)], axis=1
        ).astype(BF16)

    def from_matrix(tx, value):
        for i in range(OWN):
            tx[:, i] = value[:, i * 128 : (i + 1) * 128].reshape(NR, 8, 128).astype(BF16)

    def columns(layer):
        turn[0:8, :] = small_rx[:, layer, 0:128]
        value = turn[...].T
        for s in range(NC):
            gcol[layer, s * CH : (s + 1) * CH, :] = value[0:CH, s : s + 1]
        for k in range(2):
            for t in range(3):
                row = 3 * k + t
                turn[row : row + 1, :] = small_rx[2 * x + k, 2 + layer : 3 + layer, t * 128 : (t + 1) * 128]
        value = turn[...].T
        for row in range(6):
            bcol[layer, row * 128 : (row + 1) * 128, :] = value[:, row : row + 1]

    def weights(layer):
        for k in range(2):
            e = w_all[layer, k, :, :, 0:3].astype(F32).reshape(768, HID)
            et[layer, k * HID : (k + 1) * HID, :] = e.T.astype(BF16)
            s = w_all[layer, k, :, :, 3:6].astype(F32).reshape(768, HID)
            st[layer, :, k * HID : (k + 1) * HID] = s.astype(BF16)

    for layer in range(LAYERS):
        arrived(stats_rx.at[layer, pl.ds(0, NC - 1)], stats_r.at[layer])
        totals = jnp.sum(stats_rx[layer], axis=0)
        mean = totals[0:2] * (1.0 / 768.0)
        rstd = lax.rsqrt(totals[2:4] * (1.0 / 768.0) - mean * mean + EPS)
        pieces = []
        for hl in range(2):
            normed = ((out[hl] - mean[hl : hl + 1]) * rstd[hl : hl + 1]).astype(BF16)
            for pair in range(4):
                pieces.append(
                    jnp.concatenate(
                        [
                            normed[i * NR : (i + 1) * NR, pair * 128 : (pair + 1) * 128]
                            for i in range(OWN)
                        ],
                        axis=1,
                    )
                )
        from_matrix(there_tx.at[layer], dot(spread[...], jnp.concatenate(pieces, axis=0)))
        exchange(there_tx.at[layer], there_rx.at[layer], there_s.at[layer], there_r.at[layer])

        if layer == 0:
            arrived(small_rx.at[pl.ds(0, NC - 1)], small_r)
            wy_wait(0)
            wz_start(0, 1)
            columns(0)
            columns(1)
        else:
            wz_wait(1, 4)
            wc_copy(1).start()

        arrived(there_rx.at[layer], there_r.at[layer])
        a = dot(fwd_rows[...], as_matrix(there_rx.at[layer])).astype(BF16)
        reals, imags = [], []
        for i in range(OWN):
            at = slice(i * 128, (i + 1) * 128)
            b = dot(jnp.concatenate([a[:HALF, at], a[HALF:, at]], axis=1), fwd_lanes[...])
            b_re = b[:, :128].reshape(4, GRID, 128)
            b_im = b[:, 128:].reshape(4, GRID, 128)
            f_re = filt[layer, i, 0:GRID][None]
            f_im = filt[layer, i, GRID:][None]
            c_re = (b_re * f_re - b_im * f_im).reshape(HALF, 128)
            c_im = (b_re * f_im + b_im * f_re).reshape(HALF, 128)
            e = dot(jnp.concatenate([c_re, c_im], axis=1).astype(BF16), inv_lanes[...]).astype(BF16)
            reals.append(e[:, :128])
            imags.append(e[:, 128:])
        both = jnp.concatenate(
            [jnp.concatenate(reals, axis=1), jnp.concatenate(imags, axis=1)], axis=0
        )
        from_matrix(back_tx.at[layer], dot(inv_rows[...], both))
        exchange(back_tx.at[layer], back_rx.at[layer], back_s.at[layer], back_r.at[layer])

        if layer == 0:
            wz_wait(0, 1)
            wz_start(0, 2)
        else:
            arrived(w_all.at[1, 1 - core], wc_r.at[1])
            weights(1)

        arrived(back_rx.at[layer], back_r.at[layer])
        mixed = dot(gather[...], as_matrix(back_rx.at[layer])).astype(BF16)
        for hl in range(2):
            for pair in range(4):
                row = (hl * 4 + pair) * NR
                for i in range(OWN):
                    ag_tx[
                        layer,
                        hl,
                        pair // 2,
                        i * NR : (i + 1) * NR,
                        (pair % 2) * 128 : (pair % 2 + 1) * 128,
                    ] = mixed[row : row + NR, i * 128 : (i + 1) * 128]

        for half in range(2):

            def share(t, carry, half=half):
                to = (c + t) % NC
                pltpu.make_async_remote_copy(
                    src_ref=ag_tx.at[layer, to % 2, half],
                    dst_ref=ag_rx.at[layer, half, c],
                    send_sem=ag_s.at[layer, half],
                    recv_sem=ag_r.at[layer, half],
                    device_id=(r, to),
                    device_id_type=MESH,
                ).start()
                return carry

            lax.fori_loop(1, NC, share, 0)
            pltpu.make_async_copy(
                ag_tx.at[layer, core, half], ag_rx.at[layer, half, c], ag_r.at[layer, half]
            ).start()

        if layer == 0:
            wz_wait(0, 2)
            wz_start(0, 3)
            wz_wait(0, 3)
            wz_start(0, 4)
            wz_wait(0, 4)
            wc_copy(0).start()
            wy_wait(1)
            wz_start(1, 1)
            arrived(w_all.at[0, 1 - core], wc_r.at[0])
            weights(0)

        for half in range(2):
            arrived(ag_rx.at[layer, half], ag_r.at[layer, half])
            value = ag_rx[layer, half].astype(F32).reshape(768, HALF)
            mean = jnp.sum(value, axis=0, keepdims=True) * (1.0 / 768.0)
            square = jnp.sum(value * value, axis=0, keepdims=True) * (1.0 / 768.0)
            rstd = lax.rsqrt(square - mean * mean + EPS)
            normed2 = ((value - mean) * rstd * gcol[layer]).astype(BF16)
            hidden = jax.nn.gelu(dot(et[layer], normed2) + bcol[layer], approximate=True)
            part = dot(st[layer], hidden.astype(BF16))
            rs_tx[layer, half] = part.astype(BF16).reshape(NC, CH, HALF)

            def give(t, carry, half=half):
                to = (c + t) % NC
                pltpu.make_async_remote_copy(
                    src_ref=rs_tx.at[layer, half, to],
                    dst_ref=rs_rx.at[layer, half, c],
                    send_sem=rs_s.at[layer, half],
                    recv_sem=rs_r.at[layer, half],
                    device_id=(r, to),
                    device_id_type=MESH,
                ).start()
                return carry

            lax.fori_loop(1, NC, give, 0)
            pltpu.make_async_copy(
                rs_tx.at[layer, half, c], rs_rx.at[layer, half, c], rs_r.at[layer, half]
            ).start()

        if layer == 0:
            wz_wait(1, 1)
            wz_start(1, 2)
            wz_wait(1, 2)
            wz_start(1, 3)

        for half in range(2):
            arrived(rs_rx.at[layer, half], rs_r.at[layer, half])
            at = slice(half * HALF, (half + 1) * HALF)
            for hl in range(2):
                total = rs_rx[layer, half, hl].astype(F32)
                for chip in range(1, 4):
                    total = total + rs_rx[layer, half, 2 * chip + hl].astype(F32)
                out[hl, :, at] = out[hl, :, at] + total.astype(BF16).astype(F32)

        if layer == 0:
            put_stats(1)
            send_all(stats_rx.at[1], stats_s.at[1], stats_r.at[1])
            wz_wait(1, 3)
            wz_start(1, 4)

    arrived(small_rx.at[pl.ds(0, NC - 1)], small_s)
    for layer in range(LAYERS):
        arrived(stats_rx.at[layer, pl.ds(0, NC - 1)], stats_s.at[layer])
        arrived(there_tx.at[layer, pl.ds(0, NR - 1)], there_s.at[layer])
        arrived(back_tx.at[layer, pl.ds(0, NR - 1)], back_s.at[layer])
        for half in range(2):
            arrived(ag_rx.at[layer, half, pl.ds(0, NC - 1)], ag_s.at[layer, half])
            arrived(rs_rx.at[layer, half, pl.ds(0, NC - 1)], rs_s.at[layer, half])
        for t in range(1, NY):
            wy_copy(layer, t).wait_send()
        for step in range(1, 5):
            for way in range(2):
                wz_copy(layer, step, way).wait_send()
        wc_copy(layer).wait_send()


def per_device(tokens, spectral, gain_in, gain_mid, expand, bias, shrink):
    vmem = pl.BlockSpec(memory_space=pltpu.VMEM)
    dma = pltpu.SemaphoreType.DMA
    tables = [jnp.asarray(m) for m in matrices()]
    return pl.pallas_call(
        kernel,
        out_shape=jax.ShapeDtypeStruct(tokens.shape, F32),
        in_specs=[vmem, pl.BlockSpec(memory_space=pl.ANY)] + [vmem] * 11,
        out_specs=vmem,
        scratch_shapes=[
            pltpu.VMEM((LAYERS, OWN, GRID, 8, 128), F32),
            pltpu.VMEM((LAYERS, OWN, 128, 128), F32),
            pltpu.VMEM((NC, 4, PIX), F32),
            pltpu.VMEM((LAYERS, NC, 4, PIX), F32),
            pltpu.VMEM((LAYERS, NR, OWN, 8, 128), BF16),
            pltpu.VMEM((LAYERS, NR, OWN, 8, 128), BF16),
            pltpu.VMEM((LAYERS, NR, OWN, 8, 128), BF16),
            pltpu.VMEM((LAYERS, NR, OWN, 8, 128), BF16),
            pltpu.VMEM((LAYERS, 2, 2, CH, HALF), BF16),
            pltpu.VMEM((LAYERS, 2, NC, CH, HALF), BF16),
            pltpu.VMEM((LAYERS, 2, NC, CH, HALF), BF16),
            pltpu.VMEM((LAYERS, 2, NC, CH, HALF), BF16),
            pltpu.VMEM((LAYERS, 2, NZ, NY, 6, 8, HID), BF16),
            pltpu.VMEM((LAYERS, 768, 768), BF16),
            pltpu.VMEM((LAYERS, 768, 768), BF16),
            pltpu.VMEM((LAYERS, 768, 1), F32),
            pltpu.VMEM((LAYERS, 768, 1), F32),
            pltpu.VMEM((128, 128), F32),
            dma((LAYERS, OWN)),
            dma(()),
            dma(()),
            dma((LAYERS,)),
            dma((LAYERS,)),
            dma((LAYERS,)),
            dma((LAYERS,)),
            dma((LAYERS,)),
            dma((LAYERS,)),
            dma((LAYERS, 2)),
            dma((LAYERS, 2)),
            dma((LAYERS, 2)),
            dma((LAYERS, 2)),
            dma((LAYERS, NY)),
            dma((LAYERS, NY)),
            dma((LAYERS, 4, 2)),
            dma((LAYERS, 4, 2)),
            dma((LAYERS,)),
            dma((LAYERS,)),
        ],
        compiler_params=pltpu.CompilerParams(
            collective_id=0, has_side_effects=True, vmem_limit_bytes=56 * 1024 * 1024
        ),
        name="blocks",
    )(tokens, spectral, gain_in, gain_mid, expand, bias, shrink, *tables)


def solution(mesh):
    placed = (
        P("rows", "chan", None),
        P(None, None, "chan", None),
        P(None, "chan"),
        P(None, "chan"),
        P(None, "rows", "chan"),
        P(None, "chan"),
        P(None, "chan", "rows"),
    )
    return jax.shard_map(
        per_device, mesh=mesh, in_specs=placed, out_specs=P("rows", "chan", None), check_vma=False
    )
```

```python
import functools

import jax
import jax.numpy as jnp
import numpy as np
from jax import lax
from jax.experimental import pallas as pl
from jax.experimental.pallas import tpu as pltpu
from jax.sharding import PartitionSpec as P

MESH = pl.DeviceIdType.MESH
F32 = jnp.float32
BF16 = jnp.bfloat16

GRID = 64
LAYERS = 2
NR = 32
NC = 8
NZ, NY = 8, 4
CH = 96
OWN = 3
HID = 384
PIX = 512
NS = 2
WIDE = PIX // NS
PAIRS = WIDE // 128
PLACES = 2 * PAIRS
DEPTH = NR * PLACES
EPS = 1e-06
STOP = None


def matrices():
    index = np.arange(GRID)
    angle = 2.0 * np.pi * ((index[:, None] * index[None, :]) % GRID) / GRID
    cosine, sine = np.cos(angle), np.sin(angle)
    pairs = np.eye(PAIRS)

    def first(table):
        return np.einsum("jh,pq->pjhq", table, pairs).reshape(DEPTH, DEPTH)

    def second(table):
        return np.kron(np.eye(2), table)

    forward_rows = np.concatenate([first(cosine), -first(sine)], axis=0)
    forward_lanes = np.block([[second(cosine), -second(sine)], [second(sine), second(cosine)]])
    inverse_lanes = np.block([[second(cosine), second(sine)], [-second(sine), second(cosine)]])
    inverse_rows = np.concatenate([first(cosine).T, -first(sine).T], axis=1)
    spread = np.zeros((DEPTH, DEPTH))
    for place in range(PLACES):
        for c in range(NR):
            spread[c * PLACES + place, place * NR + c] = 1.0
    return tuple(
        np.asarray(m, dtype=jnp.bfloat16)
        for m in (forward_rows, forward_lanes, inverse_lanes, inverse_rows, spread, spread.T)
    )


def dot(a, b):
    return jnp.dot(a, b, preferred_element_type=F32)


def arrived(ref, sem):
    pltpu.make_async_copy(ref, ref, sem).wait()


def kernel(*refs):
    (
        (tokens, spectral, gain_in, gain_mid, expand, bias, shrink),
        table_hbm,
        (out,),
        table,
        (gi_buf, gm_buf, b_buf, spec_buf, filt, small_rx, stats_rx),
        (there_tx, there_rx, back_tx, back_rx, ag_tx, ag_rx, rs_tx, rs_rx),
        (w_all, et, st, gcol, bcol, turn),
        (in_sem, spec_sem, small_s, small_r, stats_s, stats_r, there_s, there_r, back_s, back_r),
        (ag_s, ag_r, rs_s, rs_r, wy_s, wy_r, wz_s, wz_r, wc_s, wc_r),
    ) = [
        tuple(refs[a:b])
        for a, b in zip((0, 7, 13, 14, 20, 27, 35, 41, 51), (7, 13, 14, 20, 27, 35, 41, 51, 61))
    ]
    fwd_rows, fwd_lanes, inv_lanes, inv_rows, spread, gather = table

    r = lax.axis_index("rows")
    c = lax.axis_index("chan")
    z, y = r // NY, r % NY
    x, core = c // 2, c % 2

    pending = {}
    leaving = []

    def owed(key):
        pending.pop(key)()

    def wait(*key):
        return lambda: owed(key)


    barrier = pltpu.get_barrier_semaphore()

    def greet_row(t, carry):
        pl.semaphore_signal(barrier, inc=1, device_id=((r + t) % NR, c), device_id_type=MESH)
        return carry

    def greet_chan(t, carry):
        pl.semaphore_signal(barrier, inc=1, device_id=(r, (c + t) % NC), device_id_type=MESH)
        return carry

    def spec_copy(layer, i):
        start = pl.multiple_of(i * NR + r // 8 * 8, 8)
        return pltpu.make_async_copy(
            spectral.at[layer, :, pl.ds(start, 8), :], spec_buf.at[layer, i], spec_sem.at[layer, i]
        )

    loads = [
        (tokens, out),
        (gain_in, gi_buf),
        (gain_mid, gm_buf),
        (bias, b_buf),
        *zip(table_hbm, table),
    ]
    for layer in range(LAYERS):
        own = w_all.at[layer, core, z, y]
        loads.append((expand.at[layer], own.at[pl.ds(0, 3)]))
        loads.append((shrink.at[layer], own.at[pl.ds(3, 3)]))
    loads = [pltpu.make_async_copy(a, b, in_sem.at[k]) for k, (a, b) in enumerate(loads)]

    def put_stats(layer, s):
        at = slice(s * WIDE, (s + 1) * WIDE)
        for hl in range(2):
            value = out[hl, :, at]
            stats_rx[layer, s, c, hl : hl + 1, :] = jnp.sum(value, axis=0, keepdims=True)
            stats_rx[layer, s, c, hl + 2 : hl + 3, :] = jnp.sum(value * value, axis=0, keepdims=True)

    def to_all(key, source, target, send, recv, whole):
        def one(t, carry):
            to = (c + t) % NC
            pltpu.make_async_remote_copy(
                src_ref=source(to),
                dst_ref=target.at[c],
                send_sem=send,
                recv_sem=recv,
                device_id=(r, to),
                device_id_type=MESH,
            ).start()
            return carry

        lax.fori_loop(1, NC, one, 0)
        if whole:
            pltpu.make_async_copy(source(c), target.at[c], recv).start()
            pending[key] = lambda: arrived(target, recv)
        else:
            pending[key] = lambda: arrived(target.at[pl.ds(0, NC - 1)], recv)
        leaving.append(lambda: arrived(target.at[pl.ds(0, NC - 1)], send))

    def send_stats(layer, s):
        put_stats(layer, s)
        buf = stats_rx.at[layer, s]
        to_all(
            ("stats", layer, s), lambda to: buf.at[c], buf, stats_s.at[layer, s], stats_r.at[layer, s], False
        )

    def enter():
        lax.fori_loop(1, NC, greet_chan, 0)
        lax.fori_loop(1, NR, greet_row, 0)
        for copy in loads:
            copy.start()
        for layer in range(LAYERS):
            for i in range(OWN):
                spec_copy(layer, i).start()
        small_rx[c] = jnp.zeros((4, PIX), F32)
        turn[...] = jnp.zeros((128, 128), F32)
        for copy in loads:
            copy.wait()
        small_rx[c, 0:2, 0:CH] = gm_buf[...]
        small_rx[c, 2:4, 0:HID] = b_buf[...].astype(F32)
        pl.semaphore_wait(barrier, NR - 1 + NC - 1)

    def send_small():
        to_all("small", lambda to: small_rx.at[c], small_rx, small_s, small_r, False)

    def filters():
        lanes = lax.broadcasted_iota(jnp.int32, (1, CH), 1)
        for layer in range(LAYERS):
            for i in range(OWN):
                spec_copy(layer, i).wait()
                values = spec_buf.at[layer, i].reshape(GRID * 8, 128)[pl.ds(r % 8, GRID, stride=8), :]
                gain = jnp.sum(
                    jnp.where(lanes == i * NR + r, gi_buf[layer : layer + 1, :], 0.0),
                    axis=1,
                    keepdims=True,
                ) * (1.0 / (GRID * GRID))
                values = values * gain
                filt[layer, i] = jnp.concatenate([values, values], axis=0).T

    def columns():
        owed("small")
        for layer in range(LAYERS):
            turn[0:8, :] = small_rx[:, layer, 0:128]
            value = turn[...].T
            for k in range(NC):
                gcol[layer, k * CH : (k + 1) * CH, :] = value[0:CH, k : k + 1]
            for k in range(2):
                for t in range(3):
                    row = 3 * k + t
                    turn[row : row + 1, :] = small_rx[
                        2 * x + k, 2 + layer : 3 + layer, t * 128 : (t + 1) * 128
                    ]
            value = turn[...].T
            for row in range(6):
                bcol[layer, row * 128 : (row + 1) * 128, :] = value[:, row : row + 1]


    def move(ref, send, recv, to, key, expected):
        copy = pltpu.make_async_remote_copy(
            src_ref=ref, dst_ref=ref, send_sem=send, recv_sem=recv, device_id=to, device_id_type=MESH
        )
        copy.start()
        leaving.append(copy.wait_send)
        earlier = pending.get(key)

        def done():
            if earlier is not None:
                earlier()
            arrived(expected, recv)

        pending[key] = done

    def wy(layer):
        ref = w_all.at[layer, core, z, y]
        for t in range(1, NY):
            move(
                ref,
                wy_s.at[layer, t],
                wy_r.at[layer, t],
                (z * NY + (y + t) % NY, c),
                ("w", layer, 0),
                w_all.at[layer, core, z, (y + NY - t) % NY],
            )

    def wz_ref(layer, step, way, shift):
        at = (z + 2 * NZ - shift) % NZ if way == 0 else (z + shift) % NZ
        ref = w_all.at[layer, core, at]
        return ref.at[pl.ds(2 * way, 2)] if step == 4 else ref

    def wz(layer, step):
        if ("w", layer, step - 1) in pending:
            owed(("w", layer, step - 1))
        for way in range(2):
            to = (z + 1) % NZ if way == 0 else (z + NZ - 1) % NZ
            move(
                wz_ref(layer, step, way, step - 1),
                wz_s.at[layer, step - 1, way],
                wz_r.at[layer, step - 1, way],
                (to * NY + y, c),
                ("w", layer, step),
                wz_ref(layer, step, way, step),
            )

    def wc(layer):
        owed(("w", layer, 4))
        move(
            w_all.at[layer, core],
            wc_s.at[layer],
            wc_r.at[layer],
            (r, x * 2 + 1 - core),
            ("w", layer, 5),
            w_all.at[layer, 1 - core],
        )

    def weights(layer):
        owed(("w", layer, 5))
        for k in range(2):
            e = w_all[layer, k, :, :, 0:3].astype(F32).reshape(768, HID)
            et[layer, k * HID : (k + 1) * HID, :] = e.T.astype(BF16)
            s = w_all[layer, k, :, :, 3:6].astype(F32).reshape(768, HID)
            st[layer, :, k * HID : (k + 1) * HID] = s.astype(BF16)


    def exchange(key, tx, rx, send, recv):
        def one(t, carry):
            to = (r + t) % NR
            pltpu.make_async_remote_copy(
                src_ref=tx.at[to],
                dst_ref=rx.at[r],
                send_sem=send,
                recv_sem=recv,
                device_id=(to, c),
                device_id_type=MESH,
            ).start()
            return carry

        lax.fori_loop(1, NR, one, 0)
        pltpu.make_async_copy(tx.at[r], rx.at[r], recv).start()
        pending[key] = lambda: arrived(rx, recv)
        leaving.append(lambda: arrived(tx.at[pl.ds(0, NR - 1)], send))

    def as_matrix(rx):
        return jnp.concatenate(
            [rx[:, i].astype(F32).reshape(DEPTH, 128) for i in range(OWN)], axis=1
        ).astype(BF16)

    def from_matrix(tx, value):
        for i in range(OWN):
            tx[:, i] = value[:, i * 128 : (i + 1) * 128].reshape(NR, PLACES, 128).astype(BF16)

    def there(layer, s):
        owed(("stats", layer, s))
        totals = jnp.sum(stats_rx[layer, s], axis=0)
        mean = totals[0:2] * (1.0 / 768.0)
        rstd = lax.rsqrt(totals[2:4] * (1.0 / 768.0) - mean * mean + EPS)
        pieces = []
        for hl in range(2):
            value = out[hl, :, s * WIDE : (s + 1) * WIDE]
            normed = ((value - mean[hl : hl + 1]) * rstd[hl : hl + 1]).astype(BF16)
            for pair in range(PAIRS):
                pieces.append(
                    jnp.concatenate(
                        [
                            normed[i * NR : (i + 1) * NR, pair * 128 : (pair + 1) * 128]
                            for i in range(OWN)
                        ],
                        axis=1,
                    )
                )
        tx = there_tx.at[layer, s]
        from_matrix(tx, dot(spread[...], jnp.concatenate(pieces, axis=0)))
        exchange(
            ("there", layer, s), tx, there_rx.at[layer, s], there_s.at[layer, s], there_r.at[layer, s]
        )

    def transform(layer, s):
        owed(("there", layer, s))
        a = dot(fwd_rows[...], as_matrix(there_rx.at[layer, s])).astype(BF16)
        reals, imags = [], []
        for i in range(OWN):
            at = slice(i * 128, (i + 1) * 128)
            b = dot(jnp.concatenate([a[:DEPTH, at], a[DEPTH:, at]], axis=1), fwd_lanes[...])
            b_re = b[:, :128].reshape(PAIRS, GRID, 128)
            b_im = b[:, 128:].reshape(PAIRS, GRID, 128)
            f_re = filt[layer, i, 0:GRID][None]
            f_im = filt[layer, i, GRID:][None]
            c_re = (b_re * f_re - b_im * f_im).reshape(DEPTH, 128)
            c_im = (b_re * f_im + b_im * f_re).reshape(DEPTH, 128)
            e = dot(jnp.concatenate([c_re, c_im], axis=1).astype(BF16), inv_lanes[...]).astype(BF16)
            reals.append(e[:, :128])
            imags.append(e[:, 128:])
        both = jnp.concatenate(
            [jnp.concatenate(reals, axis=1), jnp.concatenate(imags, axis=1)], axis=0
        )
        tx = back_tx.at[layer, s]
        from_matrix(tx, dot(inv_rows[...], both))
        exchange(
            ("back", layer, s), tx, back_rx.at[layer, s], back_s.at[layer, s], back_r.at[layer, s]
        )

    def share(layer, s):
        owed(("back", layer, s))
        mixed = dot(gather[...], as_matrix(back_rx.at[layer, s])).astype(BF16)
        for hl in range(2):
            for pair in range(PAIRS):
                row = (hl * PAIRS + pair) * NR
                for i in range(OWN):
                    ag_tx[layer, s, hl, i * NR : (i + 1) * NR, pair * 128 : (pair + 1) * 128] = mixed[
                        row : row + NR, i * 128 : (i + 1) * 128
                    ]
        to_all(
            ("ag", layer, s),
            lambda to: ag_tx.at[layer, s, to % 2],
            ag_rx.at[layer, s],
            ag_s.at[layer, s],
            ag_r.at[layer, s],
            True,
        )

    def mlp(layer, s):
        owed(("ag", layer, s))
        value = ag_rx[layer, s].astype(F32).reshape(768, WIDE)
        mean = jnp.sum(value, axis=0, keepdims=True) * (1.0 / 768.0)
        square = jnp.sum(value * value, axis=0, keepdims=True) * (1.0 / 768.0)
        rstd = lax.rsqrt(square - mean * mean + EPS)
        normed2 = ((value - mean) * rstd * gcol[layer]).astype(BF16)
        hidden = jax.nn.gelu(dot(et[layer], normed2) + bcol[layer], approximate=True)
        part = dot(st[layer], hidden.astype(BF16))
        rs_tx[layer, s] = part.astype(BF16).reshape(NC, CH, WIDE)
        to_all(
            ("rs", layer, s),
            lambda to: rs_tx.at[layer, s, to],
            rs_rx.at[layer, s],
            rs_s.at[layer, s],
            rs_r.at[layer, s],
            True,
        )

    def add(layer, s):
        owed(("rs", layer, s))
        at = slice(s * WIDE, (s + 1) * WIDE)
        for hl in range(2):
            total = rs_rx[layer, s, hl].astype(F32)
            for chip in range(1, 4):
                total = total + rs_rx[layer, s, 2 * chip + hl].astype(F32)
            out[hl, :, at] = out[hl, :, at] + total.astype(BF16).astype(F32)
        if layer + 1 < LAYERS:
            send_stats(layer + 1, s)


    plan = [("enter", enter)]

    def then(name, f, *args):
        plan.append((f"{name} {args}", functools.partial(f, *args)))

    def each(name, f, layer):
        for s in range(NS):
            then(name, f, layer, s)

    each("stats", send_stats, 0)
    then("wy", wy, 0)
    then("small", send_small)
    then("filters", filters)
    then("wz", wz, 0, 1)
    each("there", there, 0)
    then("columns", columns)
    each("transform", transform, 0)
    then("wz", wz, 0, 2)
    then("wy", wy, 1)
    each("share", share, 0)
    then("wz", wz, 0, 3)
    then("wz", wz, 0, 4)
    then("wc", wc, 0)
    then("wz", wz, 1, 1)
    then("weights", weights, 0)
    each("mlp", mlp, 0)
    then("wz", wz, 1, 2)
    then("wz", wz, 1, 3)
    each("add", add, 0)
    then("wz", wz, 1, 4)
    each("there", there, 1)
    then("wc", wc, 1)
    each("transform", transform, 1)
    then("weights", weights, 1)
    each("share", share, 1)
    each("mlp", mlp, 1)
    each("add", add, 1)

    for _, step in plan[:STOP]:
        step()
    for key in list(pending):
        owed(key)
    for done in leaving:
        done()


def per_device(tokens, spectral, gain_in, gain_mid, expand, bias, shrink):
    hbm = pl.BlockSpec(memory_space=pl.ANY)
    dma = pltpu.SemaphoreType.DMA
    tables = [jnp.asarray(m) for m in matrices()]
    message = (LAYERS, NS, NR, OWN, PLACES, 128)
    scratch = [pltpu.VMEM(m.shape, BF16) for m in tables]
    scratch += [
        pltpu.VMEM((LAYERS, CH), F32),
        pltpu.VMEM((LAYERS, CH), F32),
        pltpu.VMEM((LAYERS, HID), BF16),
        pltpu.VMEM((LAYERS, OWN, GRID, 8, 128), F32),
        pltpu.VMEM((LAYERS, OWN, 128, 128), F32),
        pltpu.VMEM((NC, 4, PIX), F32),
        pltpu.VMEM((LAYERS, NS, NC, 4, WIDE), F32),
        pltpu.VMEM(message, BF16),
        pltpu.VMEM(message, BF16),
        pltpu.VMEM(message, BF16),
        pltpu.VMEM(message, BF16),
        pltpu.VMEM((LAYERS, NS, 2, CH, WIDE), BF16),
        pltpu.VMEM((LAYERS, NS, NC, CH, WIDE), BF16),
        pltpu.VMEM((LAYERS, NS, NC, CH, WIDE), BF16),
        pltpu.VMEM((LAYERS, NS, NC, CH, WIDE), BF16),
        pltpu.VMEM((LAYERS, 2, NZ, NY, 6, 8, HID), BF16),
        pltpu.VMEM((LAYERS, 768, 768), BF16),
        pltpu.VMEM((LAYERS, 768, 768), BF16),
        pltpu.VMEM((LAYERS, 768, 1), F32),
        pltpu.VMEM((LAYERS, 768, 1), F32),
        pltpu.VMEM((128, 128), F32),
        dma((14,)),
        dma((LAYERS, OWN)),
        dma(()),
        dma(()),
    ]
    scratch += [dma((LAYERS, NS))] * 10
    scratch += [dma((LAYERS, NY))] * 2 + [dma((LAYERS, 4, 2))] * 2 + [dma((LAYERS,))] * 2
    return pl.pallas_call(
        kernel,
        out_shape=jax.ShapeDtypeStruct(tokens.shape, F32),
        in_specs=[hbm] * 13,
        out_specs=pl.BlockSpec(memory_space=pltpu.VMEM),
        scratch_shapes=scratch,
        compiler_params=pltpu.CompilerParams(
            collective_id=0, has_side_effects=True, vmem_limit_bytes=56 * 1024 * 1024
        ),
        name="blocks",
    )(
        tokens,
        spectral,
        gain_in,
        gain_mid,
        expand.reshape(LAYERS, 3, 8, HID),
        bias,
        shrink.transpose(0, 2, 1).reshape(LAYERS, 3, 8, HID),
        *tables,
    )


def solution(mesh):
    placed = (
        P("rows", "chan", None),
        P(None, None, "chan", None),
        P(None, "chan"),
        P(None, "chan"),
        P(None, "rows", "chan"),
        P(None, "chan"),
        P(None, "chan", "rows"),
    )
    return jax.shard_map(
        per_device, mesh=mesh, in_specs=placed, out_specs=P("rows", "chan", None), check_vma=False
    )
```

```python
import functools

import jax
import jax.numpy as jnp
import numpy as np
from jax import lax
from jax.experimental import pallas as pl
from jax.experimental.pallas import tpu as pltpu
from jax.sharding import PartitionSpec as P

MESH = pl.DeviceIdType.MESH
F32 = jnp.float32
BF16 = jnp.bfloat16

GRID = 64
LAYERS = 2
NR = 32
NC = 8
NZ, NY = 8, 4
CH = 96
OWN = 3
HID = 384
PIX = 512
NS = 2
WIDE = PIX // NS
PAIRS = WIDE // 128
PLACES = 2 * PAIRS
DEPTH = NR * PLACES
EPS = 1e-06
STOP = None


def matrices():
    index = np.arange(GRID)
    angle = 2.0 * np.pi * ((index[:, None] * index[None, :]) % GRID) / GRID
    cosine, sine = np.cos(angle), np.sin(angle)
    pairs = np.eye(PAIRS)

    def first(table):
        return np.einsum("jh,pq->pjhq", table, pairs).reshape(DEPTH, DEPTH)

    def second(table):
        return np.kron(np.eye(2), table)

    forward_rows = np.concatenate([first(cosine), -first(sine)], axis=0)
    forward_lanes = np.block([[second(cosine), -second(sine)], [second(sine), second(cosine)]])
    inverse_lanes = np.block([[second(cosine), second(sine)], [-second(sine), second(cosine)]])
    inverse_rows = np.concatenate([first(cosine).T, -first(sine).T], axis=1)
    spread = np.zeros((DEPTH, DEPTH))
    for place in range(PLACES):
        for c in range(NR):
            spread[c * PLACES + place, place * NR + c] = 1.0
    return tuple(
        np.asarray(m, dtype=jnp.bfloat16)
        for m in (forward_rows, forward_lanes, inverse_lanes, inverse_rows, spread, spread.T)
    )


def dot(a, b):
    return jnp.dot(a, b, preferred_element_type=F32)


def arrived(ref, sem):
    pltpu.make_async_copy(ref, ref, sem).wait()


def kernel(*refs):
    (
        (tokens, spectral, gain_in, gain_mid, expand, bias, shrink),
        table_hbm,
        (out,),
        table,
        (gi_buf, gm_buf, b_buf, spec_buf, filt, small_rx, stats_rx),
        (there_tx, there_rx, back_tx, back_rx, ag_tx, ag_rx, rs_tx, rs_rx),
        (w_all, et, st, gcol, bcol, turn),
        (in_sem, spec_sem, small_s, small_r, stats_s, stats_r, there_s, there_r, back_s, back_r),
        (ag_s, ag_r, rs_s, rs_r, wy_s, wy_r, wz_s, wz_r, wc_s, wc_r, near_sem, far_sem),
    ) = [
        tuple(refs[a:b])
        for a, b in zip((0, 7, 13, 14, 20, 27, 35, 41, 51), (7, 13, 14, 20, 27, 35, 41, 51, 63))
    ]
    fwd_rows, fwd_lanes, inv_lanes, inv_rows, spread, gather = table

    r = lax.axis_index("rows")
    c = lax.axis_index("chan")
    z, y = r // NY, r % NY
    x, core = c // 2, c % 2

    pending = {}
    leaving = []

    def owed(key):
        pending.pop(key)()

    def wait(*key):
        return lambda: owed(key)


    barrier = pltpu.get_barrier_semaphore()

    def greet_rows(sem, shifts_z, shifts_y=()):
        for t in shifts_z:
            pl.semaphore_signal(
                sem, inc=1, device_id=((z + NZ + t) % NZ * NY + y, c), device_id_type=MESH
            )
        for t in shifts_y:
            pl.semaphore_signal(
                sem, inc=1, device_id=(z * NY + (y + t) % NY, c), device_id_type=MESH
            )

    def greet_chan(t, carry):
        pl.semaphore_signal(barrier, inc=1, device_id=(r, (c + t) % NC), device_id_type=MESH)
        return carry

    def spec_copy(layer, i):
        start = pl.multiple_of(i * NR + r // 8 * 8, 8)
        return pltpu.make_async_copy(
            spectral.at[layer, :, pl.ds(start, 8), :], spec_buf.at[layer, i], spec_sem.at[layer, i]
        )

    loads = [
        (tokens, out),
        (gain_in, gi_buf),
        (gain_mid, gm_buf),
        (bias, b_buf),
        *zip(table_hbm, table),
    ]
    for layer in range(LAYERS):
        own = w_all.at[layer, core, z, y]
        loads.append((expand.at[layer], own.at[pl.ds(0, 3)]))
        loads.append((shrink.at[layer], own.at[pl.ds(3, 3)]))
    loads = [pltpu.make_async_copy(a, b, in_sem.at[k]) for k, (a, b) in enumerate(loads)]

    def put_stats(layer, s):
        at = slice(s * WIDE, (s + 1) * WIDE)
        for hl in range(2):
            value = out[hl, :, at]
            stats_rx[layer, s, c, hl : hl + 1, :] = jnp.sum(value, axis=0, keepdims=True)
            stats_rx[layer, s, c, hl + 2 : hl + 3, :] = jnp.sum(value * value, axis=0, keepdims=True)

    def to_all(key, source, target, send, recv, whole):
        def one(t, carry):
            to = (c + t) % NC
            pltpu.make_async_remote_copy(
                src_ref=source(to),
                dst_ref=target.at[c],
                send_sem=send,
                recv_sem=recv,
                device_id=(r, to),
                device_id_type=MESH,
            ).start()
            return carry

        lax.fori_loop(1, NC, one, 0)
        if whole:
            pltpu.make_async_copy(source(c), target.at[c], recv).start()
            pending[key] = lambda: arrived(target, recv)
        else:
            pending[key] = lambda: arrived(target.at[pl.ds(0, NC - 1)], recv)
        leaving.append(lambda: arrived(target.at[pl.ds(0, NC - 1)], send))

    def send_stats(layer, s):
        put_stats(layer, s)
        buf = stats_rx.at[layer, s]
        to_all(
            ("stats", layer, s), lambda to: buf.at[c], buf, stats_s.at[layer, s], stats_r.at[layer, s], False
        )

    def enter():
        lax.fori_loop(1, NC, greet_chan, 0)
        greet_rows(barrier, (-2, -1, 1, 2), (1, 2, 3))
        for copy in loads:
            copy.start()
        for layer in range(LAYERS):
            for i in range(OWN):
                spec_copy(layer, i).start()
                pending["spec", layer, i] = spec_copy(layer, i).wait
        small_rx[c] = jnp.zeros((4, PIX), F32)
        turn[...] = jnp.zeros((128, 128), F32)
        for copy in loads:
            copy.wait()
        small_rx[c, 0:2, 0:CH] = gm_buf[...]
        small_rx[c, 2:4, 0:HID] = b_buf[...].astype(F32)
        pl.semaphore_wait(barrier, NC - 1 + 7)
        greet_rows(near_sem, (-2, -1, 1, 2))


    def hear_near():
        pl.semaphore_wait(near_sem, 4)
        greet_rows(far_sem, (-2, 2))

    def hear_far():
        pl.semaphore_wait(far_sem, 2)

    def send_small():
        to_all("small", lambda to: small_rx.at[c], small_rx, small_s, small_r, False)

    def filters():
        lanes = lax.broadcasted_iota(jnp.int32, (1, CH), 1)
        for layer in range(LAYERS):
            for i in range(OWN):
                owed(("spec", layer, i))
                values = spec_buf.at[layer, i].reshape(GRID * 8, 128)[pl.ds(r % 8, GRID, stride=8), :]
                gain = jnp.sum(
                    jnp.where(lanes == i * NR + r, gi_buf[layer : layer + 1, :], 0.0),
                    axis=1,
                    keepdims=True,
                ) * (1.0 / (GRID * GRID))
                values = values * gain
                filt[layer, i] = jnp.concatenate([values, values], axis=0).T

    def columns():
        owed("small")
        for layer in range(LAYERS):
            turn[0:8, :] = small_rx[:, layer, 0:128]
            value = turn[...].T
            for k in range(NC):
                gcol[layer, k * CH : (k + 1) * CH, :] = value[0:CH, k : k + 1]
            for k in range(2):
                for t in range(3):
                    row = 3 * k + t
                    turn[row : row + 1, :] = small_rx[
                        2 * x + k, 2 + layer : 3 + layer, t * 128 : (t + 1) * 128
                    ]
            value = turn[...].T
            for row in range(6):
                bcol[layer, row * 128 : (row + 1) * 128, :] = value[:, row : row + 1]


    def move(ref, send, recv, to, key, expected):
        copy = pltpu.make_async_remote_copy(
            src_ref=ref, dst_ref=ref, send_sem=send, recv_sem=recv, device_id=to, device_id_type=MESH
        )
        copy.start()
        leaving.append(copy.wait_send)
        earlier = pending.get(key)

        def done():
            if earlier is not None:
                earlier()
            arrived(expected, recv)

        pending[key] = done

    def wy(layer):
        ref = w_all.at[layer, core, z, y]
        for t in range(1, NY):
            move(
                ref,
                wy_s.at[layer, t],
                wy_r.at[layer, t],
                (z * NY + (y + t) % NY, c),
                ("w", layer, 0),
                w_all.at[layer, core, z, (y + NY - t) % NY],
            )

    def wz_ref(layer, step, way, shift):
        at = (z + 2 * NZ - shift) % NZ if way == 0 else (z + shift) % NZ
        ref = w_all.at[layer, core, at]
        return ref.at[pl.ds(2 * way, 2)] if step == 4 else ref

    def wz(layer, step):
        if ("w", layer, step - 1) in pending:
            owed(("w", layer, step - 1))
        for way in range(2):
            to = (z + 1) % NZ if way == 0 else (z + NZ - 1) % NZ
            move(
                wz_ref(layer, step, way, step - 1),
                wz_s.at[layer, step - 1, way],
                wz_r.at[layer, step - 1, way],
                (to * NY + y, c),
                ("w", layer, step),
                wz_ref(layer, step, way, step),
            )

    def wc(layer):
        owed(("w", layer, 4))
        move(
            w_all.at[layer, core],
            wc_s.at[layer],
            wc_r.at[layer],
            (r, x * 2 + 1 - core),
            ("w", layer, 5),
            w_all.at[layer, 1 - core],
        )

    def weights(layer):
        owed(("w", layer, 5))
        for k in range(2):
            e = w_all[layer, k, :, :, 0:3].astype(F32).reshape(768, HID)
            et[layer, k * HID : (k + 1) * HID, :] = e.T.astype(BF16)
            s = w_all[layer, k, :, :, 3:6].astype(F32).reshape(768, HID)
            st[layer, :, k * HID : (k + 1) * HID] = s.astype(BF16)


    def exchange(key, tx, rx, send, recv):
        def one(t, carry):
            to = (r + t) % NR
            pltpu.make_async_remote_copy(
                src_ref=tx.at[to],
                dst_ref=rx.at[r],
                send_sem=send,
                recv_sem=recv,
                device_id=(to, c),
                device_id_type=MESH,
            ).start()
            return carry

        lax.fori_loop(1, NR, one, 0)
        pltpu.make_async_copy(tx.at[r], rx.at[r], recv).start()
        pending[key] = lambda: arrived(rx, recv)
        leaving.append(lambda: arrived(tx.at[pl.ds(0, NR - 1)], send))

    def as_matrix(rx):
        return jnp.concatenate(
            [rx[:, i].astype(F32).reshape(DEPTH, 128) for i in range(OWN)], axis=1
        ).astype(BF16)

    def from_matrix(tx, value):
        for i in range(OWN):
            tx[:, i] = value[:, i * 128 : (i + 1) * 128].reshape(NR, PLACES, 128).astype(BF16)

    def there(layer, s):
        owed(("stats", layer, s))
        totals = jnp.sum(stats_rx[layer, s], axis=0)
        mean = totals[0:2] * (1.0 / 768.0)
        rstd = lax.rsqrt(totals[2:4] * (1.0 / 768.0) - mean * mean + EPS)
        pieces = []
        for hl in range(2):
            value = out[hl, :, s * WIDE : (s + 1) * WIDE]
            normed = ((value - mean[hl : hl + 1]) * rstd[hl : hl + 1]).astype(BF16)
            for pair in range(PAIRS):
                pieces.append(
                    jnp.concatenate(
                        [
                            normed[i * NR : (i + 1) * NR, pair * 128 : (pair + 1) * 128]
                            for i in range(OWN)
                        ],
                        axis=1,
                    )
                )
        tx = there_tx.at[layer, s]
        from_matrix(tx, dot(spread[...], jnp.concatenate(pieces, axis=0)))
        exchange(
            ("there", layer, s), tx, there_rx.at[layer, s], there_s.at[layer, s], there_r.at[layer, s]
        )

    def transform(layer, s):
        owed(("there", layer, s))
        a = dot(fwd_rows[...], as_matrix(there_rx.at[layer, s])).astype(BF16)
        reals, imags = [], []
        for i in range(OWN):
            at = slice(i * 128, (i + 1) * 128)
            b = dot(jnp.concatenate([a[:DEPTH, at], a[DEPTH:, at]], axis=1), fwd_lanes[...])
            b_re = b[:, :128].reshape(PAIRS, GRID, 128)
            b_im = b[:, 128:].reshape(PAIRS, GRID, 128)
            f_re = filt[layer, i, 0:GRID][None]
            f_im = filt[layer, i, GRID:][None]
            c_re = (b_re * f_re - b_im * f_im).reshape(DEPTH, 128)
            c_im = (b_re * f_im + b_im * f_re).reshape(DEPTH, 128)
            e = dot(jnp.concatenate([c_re, c_im], axis=1).astype(BF16), inv_lanes[...]).astype(BF16)
            reals.append(e[:, :128])
            imags.append(e[:, 128:])
        both = jnp.concatenate(
            [jnp.concatenate(reals, axis=1), jnp.concatenate(imags, axis=1)], axis=0
        )
        tx = back_tx.at[layer, s]
        from_matrix(tx, dot(inv_rows[...], both))
        exchange(
            ("back", layer, s), tx, back_rx.at[layer, s], back_s.at[layer, s], back_r.at[layer, s]
        )

    def share(layer, s):
        owed(("back", layer, s))
        mixed = dot(gather[...], as_matrix(back_rx.at[layer, s])).astype(BF16)
        for hl in range(2):
            for pair in range(PAIRS):
                row = (hl * PAIRS + pair) * NR
                for i in range(OWN):
                    ag_tx[layer, s, hl, i * NR : (i + 1) * NR, pair * 128 : (pair + 1) * 128] = mixed[
                        row : row + NR, i * 128 : (i + 1) * 128
                    ]
        to_all(
            ("ag", layer, s),
            lambda to: ag_tx.at[layer, s, to % 2],
            ag_rx.at[layer, s],
            ag_s.at[layer, s],
            ag_r.at[layer, s],
            True,
        )

    def mlp(layer, s):
        owed(("ag", layer, s))
        value = ag_rx[layer, s].astype(F32).reshape(768, WIDE)
        mean = jnp.sum(value, axis=0, keepdims=True) * (1.0 / 768.0)
        square = jnp.sum(value * value, axis=0, keepdims=True) * (1.0 / 768.0)
        rstd = lax.rsqrt(square - mean * mean + EPS)
        normed2 = ((value - mean) * rstd * gcol[layer]).astype(BF16)
        hidden = jax.nn.gelu(dot(et[layer], normed2) + bcol[layer], approximate=True)
        part = dot(st[layer], hidden.astype(BF16))
        rs_tx[layer, s] = part.astype(BF16).reshape(NC, CH, WIDE)
        to_all(
            ("rs", layer, s),
            lambda to: rs_tx.at[layer, s, to],
            rs_rx.at[layer, s],
            rs_s.at[layer, s],
            rs_r.at[layer, s],
            True,
        )

    def add(layer, s):
        owed(("rs", layer, s))
        at = slice(s * WIDE, (s + 1) * WIDE)
        for hl in range(2):
            total = rs_rx[layer, s, hl].astype(F32)
            for chip in range(1, 4):
                total = total + rs_rx[layer, s, 2 * chip + hl].astype(F32)
            out[hl, :, at] = out[hl, :, at] + total.astype(BF16).astype(F32)
        if layer + 1 < LAYERS:
            send_stats(layer + 1, s)


    plan = [("enter", enter)]

    def then(name, f, *args):
        plan.append((f"{name} {args}", functools.partial(f, *args)))

    def each(name, f, layer):
        for s in range(NS):
            then(name, f, layer, s)

    each("stats", send_stats, 0)
    then("near", hear_near)
    then("wy", wy, 0)
    then("small", send_small)
    then("wy", wy, 1)
    then("filters", filters)
    then("far", hear_far)
    then("wz", wz, 0, 1)
    each("there", there, 0)
    then("columns", columns)
    then("wz", wz, 0, 2)
    each("transform", transform, 0)
    then("wz", wz, 0, 3)
    then("wz", wz, 0, 4)
    each("share", share, 0)
    then("wc", wc, 0)
    then("wz", wz, 1, 1)
    then("weights", weights, 0)
    each("mlp", mlp, 0)
    then("wz", wz, 1, 2)
    then("wz", wz, 1, 3)
    each("add", add, 0)
    then("wz", wz, 1, 4)
    each("there", there, 1)
    then("wc", wc, 1)
    each("transform", transform, 1)
    then("weights", weights, 1)
    each("share", share, 1)
    each("mlp", mlp, 1)
    each("add", add, 1)

    for _, step in plan[:STOP]:
        step()
    for key in list(pending):
        owed(key)
    for done in leaving:
        done()


def per_device(tokens, spectral, gain_in, gain_mid, expand, bias, shrink):
    hbm = pl.BlockSpec(memory_space=pl.ANY)
    dma = pltpu.SemaphoreType.DMA
    tables = [jnp.asarray(m) for m in matrices()]
    message = (LAYERS, NS, NR, OWN, PLACES, 128)
    scratch = [pltpu.VMEM(m.shape, BF16) for m in tables]
    scratch += [
        pltpu.VMEM((LAYERS, CH), F32),
        pltpu.VMEM((LAYERS, CH), F32),
        pltpu.VMEM((LAYERS, HID), BF16),
        pltpu.VMEM((LAYERS, OWN, GRID, 8, 128), F32),
        pltpu.VMEM((LAYERS, OWN, 128, 128), F32),
        pltpu.VMEM((NC, 4, PIX), F32),
        pltpu.VMEM((LAYERS, NS, NC, 4, WIDE), F32),
        pltpu.VMEM(message, BF16),
        pltpu.VMEM(message, BF16),
        pltpu.VMEM(message, BF16),
        pltpu.VMEM(message, BF16),
        pltpu.VMEM((LAYERS, NS, 2, CH, WIDE), BF16),
        pltpu.VMEM((LAYERS, NS, NC, CH, WIDE), BF16),
        pltpu.VMEM((LAYERS, NS, NC, CH, WIDE), BF16),
        pltpu.VMEM((LAYERS, NS, NC, CH, WIDE), BF16),
        pltpu.VMEM((LAYERS, 2, NZ, NY, 6, 8, HID), BF16),
        pltpu.VMEM((LAYERS, 768, 768), BF16),
        pltpu.VMEM((LAYERS, 768, 768), BF16),
        pltpu.VMEM((LAYERS, 768, 1), F32),
        pltpu.VMEM((LAYERS, 768, 1), F32),
        pltpu.VMEM((128, 128), F32),
        dma((14,)),
        dma((LAYERS, OWN)),
        dma(()),
        dma(()),
    ]
    scratch += [dma((LAYERS, NS))] * 10
    scratch += [dma((LAYERS, NY))] * 2 + [dma((LAYERS, 4, 2))] * 2 + [dma((LAYERS,))] * 2
    scratch += [pltpu.SemaphoreType.REGULAR] * 2
    return pl.pallas_call(
        kernel,
        out_shape=pltpu.VMEM(tokens.shape, F32),
        in_specs=[hbm] * 13,
        out_specs=pl.BlockSpec(memory_space=pltpu.VMEM),
        scratch_shapes=scratch,
        compiler_params=pltpu.CompilerParams(
            collective_id=0, has_side_effects=True, vmem_limit_bytes=56 * 1024 * 1024
        ),
        name="blocks",
    )(
        tokens,
        spectral,
        gain_in,
        gain_mid,
        expand.reshape(LAYERS, 3, 8, HID),
        bias,
        shrink.transpose(0, 2, 1).reshape(LAYERS, 3, 8, HID),
        *tables,
    )


def solution(mesh):
    placed = (
        P("rows", "chan", None),
        P(None, None, "chan", None),
        P(None, "chan"),
        P(None, "chan"),
        P(None, "rows", "chan"),
        P(None, "chan"),
        P(None, "chan", "rows"),
    )
    return jax.shard_map(
        per_device, mesh=mesh, in_specs=placed, out_specs=P("rows", "chan", None), check_vma=False
    )
```

```python
import functools

import jax
import jax.numpy as jnp
import numpy as np
from jax import lax
from jax.experimental import pallas as pl
from jax.experimental.pallas import tpu as pltpu
from jax.sharding import PartitionSpec as P

MESH = pl.DeviceIdType.MESH
F32 = jnp.float32
BF16 = jnp.bfloat16

GRID = 64
LAYERS = 2
NR = 32
NC = 8
NZ, NY = 8, 4
CH = 96
OWN = 3
HID = 384
PIX = 512
NS = 2
WIDE = PIX // NS
PAIRS = WIDE // 128
PLACES = 2 * PAIRS
DEPTH = NR * PLACES
EPS = 1e-06
STOP = None


def matrices():
    index = np.arange(GRID)
    angle = 2.0 * np.pi * ((index[:, None] * index[None, :]) % GRID) / GRID
    cosine, sine = np.cos(angle), np.sin(angle)
    pairs = np.eye(PAIRS)

    def first(table):
        return np.einsum("jh,pq->pjhq", table, pairs).reshape(DEPTH, DEPTH)

    def second(table):
        return np.kron(np.eye(2), table)

    forward_rows = np.concatenate([first(cosine), -first(sine)], axis=0)
    forward_lanes = np.block([[second(cosine), -second(sine)], [second(sine), second(cosine)]])
    inverse_lanes = np.block([[second(cosine), second(sine)], [-second(sine), second(cosine)]])
    inverse_rows = np.concatenate([first(cosine).T, -first(sine).T], axis=1)
    spread = np.zeros((DEPTH, DEPTH))
    for place in range(PLACES):
        for c in range(NR):
            spread[c * PLACES + place, place * NR + c] = 1.0
    return tuple(
        np.asarray(m, dtype=jnp.bfloat16)
        for m in (forward_rows, forward_lanes, inverse_lanes, inverse_rows, spread, spread.T)
    )


def dot(a, b):
    return jnp.dot(a, b, preferred_element_type=F32)


def arrived(ref, sem):
    pltpu.make_async_copy(ref, ref, sem).wait()


def kernel(*refs):
    (
        (tokens, spectral, gain_in, gain_mid, expand, bias, shrink),
        table_hbm,
        (out,),
        table,
        (gi_buf, gm_buf, b_buf, spec_buf, filt, small_rx, stats_rx),
        (there_tx, there_rx, back_tx, back_rx, ag_tx, ag_rx, rs_tx, rs_rx, rl_tx, rl_rx),
        (w_all, et, st, gcol, bcol, turn),
        (in_sem, spec_sem, small_s, small_r, stats_s, stats_r, there_s, there_r, back_s, back_r),
        (ag_s, ag_r, rs_s, rs_r, wy_s, wy_r, wz_s, wz_r, wc_s, wc_r, near_sem, far_sem),
    ) = [
        tuple(refs[a:b])
        for a, b in zip((0, 7, 13, 14, 20, 27, 37, 43, 53), (7, 13, 14, 20, 27, 37, 43, 53, 65))
    ]
    fwd_rows, fwd_lanes, inv_lanes, inv_rows, spread, gather = table

    r = lax.axis_index("rows")
    c = lax.axis_index("chan")
    z, y = r // NY, r % NY
    x, core = c // 2, c % 2
    above, below, across = (x + 1) % 4, (x + 3) % 4, (x + 2) % 4
    halves = (pl.ds(0, CH // 2), pl.ds(CH // 2, CH // 2))

    pending = {}
    leaving = []

    def owed(key):
        pending.pop(key)()

    def wait(*key):
        return lambda: owed(key)

    def remote(src, dst, send, recv, to):
        pltpu.make_async_remote_copy(
            src_ref=src, dst_ref=dst, send_sem=send, recv_sem=recv, device_id=(r, to), device_id_type=MESH
        ).start()


    barrier = pltpu.get_barrier_semaphore()

    def greet_rows(sem, shifts_z, shifts_y=()):
        for t in shifts_z:
            pl.semaphore_signal(
                sem, inc=1, device_id=((z + NZ + t) % NZ * NY + y, c), device_id_type=MESH
            )
        for t in shifts_y:
            pl.semaphore_signal(
                sem, inc=1, device_id=(z * NY + (y + t) % NY, c), device_id_type=MESH
            )

    def greet_chan(t, carry):
        pl.semaphore_signal(barrier, inc=1, device_id=(r, (c + t) % NC), device_id_type=MESH)
        return carry

    def spec_copy(layer, i):
        start = pl.multiple_of(i * NR + r // 8 * 8, 8)
        return pltpu.make_async_copy(
            spectral.at[layer, :, pl.ds(start, 8), :], spec_buf.at[layer, i], spec_sem.at[layer, i]
        )

    loads = [
        (tokens, out),
        (gain_in, gi_buf),
        (gain_mid, gm_buf),
        (bias, b_buf),
        *zip(table_hbm, table),
    ]
    for layer in range(LAYERS):
        own = w_all.at[layer, core, z, y]
        loads.append((expand.at[layer], own.at[pl.ds(0, 3)]))
        loads.append((shrink.at[layer], own.at[pl.ds(3, 3)]))
    loads = [pltpu.make_async_copy(a, b, in_sem.at[k]) for k, (a, b) in enumerate(loads)]

    def put_stats(layer, s):
        at = slice(s * WIDE, (s + 1) * WIDE)
        for hl in range(2):
            value = out[hl, :, at]
            stats_rx[layer, s, c, hl : hl + 1, :] = jnp.sum(value, axis=0, keepdims=True)
            stats_rx[layer, s, c, hl + 2 : hl + 3, :] = jnp.sum(value * value, axis=0, keepdims=True)

    def to_all(key, target, send, recv):
        def one(t, carry):
            to = (c + t) % NC
            pltpu.make_async_remote_copy(
                src_ref=target.at[c],
                dst_ref=target.at[c],
                send_sem=send,
                recv_sem=recv,
                device_id=(r, to),
                device_id_type=MESH,
            ).start()
            return carry

        lax.fori_loop(1, NC, one, 0)
        pending[key] = lambda: arrived(target.at[pl.ds(0, NC - 1)], recv)
        leaving.append(lambda: arrived(target.at[pl.ds(0, NC - 1)], send))

    def send_stats(layer, s):
        put_stats(layer, s)
        buf = stats_rx.at[layer, s]
        to_all(("stats", layer, s), buf, stats_s.at[layer, s], stats_r.at[layer, s])

    def enter():
        lax.fori_loop(1, NC, greet_chan, 0)
        greet_rows(barrier, (-2, -1, 1, 2), (1, 2, 3))
        for copy in loads:
            copy.start()
        for layer in range(LAYERS):
            for i in range(OWN):
                spec_copy(layer, i).start()
                pending["spec", layer, i] = spec_copy(layer, i).wait
        small_rx[c] = jnp.zeros((4, PIX), F32)
        turn[...] = jnp.zeros((128, 128), F32)
        for copy in loads:
            copy.wait()
        small_rx[c, 0:2, 0:CH] = gm_buf[...]
        small_rx[c, 2:4, 0:HID] = b_buf[...].astype(F32)
        pl.semaphore_wait(barrier, NC - 1 + 7)
        greet_rows(near_sem, (-2, -1, 1, 2))


    def hear_near():
        pl.semaphore_wait(near_sem, 4)
        greet_rows(far_sem, (-2, 2))

    def hear_far():
        pl.semaphore_wait(far_sem, 2)

    def send_small():
        to_all("small", small_rx, small_s, small_r)

    def filters():
        lanes = lax.broadcasted_iota(jnp.int32, (1, CH), 1)
        for layer in range(LAYERS):
            for i in range(OWN):
                owed(("spec", layer, i))
                values = spec_buf.at[layer, i].reshape(GRID * 8, 128)[pl.ds(r % 8, GRID, stride=8), :]
                gain = jnp.sum(
                    jnp.where(lanes == i * NR + r, gi_buf[layer : layer + 1, :], 0.0),
                    axis=1,
                    keepdims=True,
                ) * (1.0 / (GRID * GRID))
                values = values * gain
                filt[layer, i] = jnp.concatenate([values, values], axis=0).T

    def columns():
        owed("small")
        for layer in range(LAYERS):
            turn[0:8, :] = small_rx[:, layer, 0:128]
            value = turn[...].T
            for k in range(NC):
                gcol[layer, k * CH : (k + 1) * CH, :] = value[0:CH, k : k + 1]
            for k in range(2):
                for t in range(3):
                    row = 3 * k + t
                    turn[row : row + 1, :] = small_rx[
                        2 * x + k, 2 + layer : 3 + layer, t * 128 : (t + 1) * 128
                    ]
            value = turn[...].T
            for row in range(6):
                bcol[layer, row * 128 : (row + 1) * 128, :] = value[:, row : row + 1]


    def move(ref, send, recv, to, key, expected):
        copy = pltpu.make_async_remote_copy(
            src_ref=ref, dst_ref=ref, send_sem=send, recv_sem=recv, device_id=to, device_id_type=MESH
        )
        copy.start()
        leaving.append(copy.wait_send)
        earlier = pending.get(key)

        def done():
            if earlier is not None:
                earlier()
            arrived(expected, recv)

        pending[key] = done

    def wy(layer):
        ref = w_all.at[layer, core, z, y]
        for t in range(1, NY):
            move(
                ref,
                wy_s.at[layer, t],
                wy_r.at[layer, t],
                (z * NY + (y + t) % NY, c),
                ("w", layer, 0),
                w_all.at[layer, core, z, (y + NY - t) % NY],
            )

    def wz_ref(layer, step, way, shift):
        at = (z + 2 * NZ - shift) % NZ if way == 0 else (z + shift) % NZ
        ref = w_all.at[layer, core, at]
        return ref.at[pl.ds(2 * way, 2)] if step == 4 else ref

    def wz(layer, step):
        if ("w", layer, step - 1) in pending:
            owed(("w", layer, step - 1))
        for way in range(2):
            to = (z + 1) % NZ if way == 0 else (z + NZ - 1) % NZ
            move(
                wz_ref(layer, step, way, step - 1),
                wz_s.at[layer, step - 1, way],
                wz_r.at[layer, step - 1, way],
                (to * NY + y, c),
                ("w", layer, step),
                wz_ref(layer, step, way, step),
            )

    def wc(layer):
        owed(("w", layer, 4))
        move(
            w_all.at[layer, core],
            wc_s.at[layer],
            wc_r.at[layer],
            (r, x * 2 + 1 - core),
            ("w", layer, 5),
            w_all.at[layer, 1 - core],
        )

    def weights(layer):
        owed(("w", layer, 5))
        for k in range(2):
            e = w_all[layer, k, :, :, 0:3].astype(F32).reshape(768, HID)
            et[layer, k * HID : (k + 1) * HID, :] = e.T.astype(BF16)
            s = w_all[layer, k, :, :, 3:6].astype(F32).reshape(768, HID)
            st[layer, :, k * HID : (k + 1) * HID] = s.astype(BF16)


    def exchange(key, tx, rx, send, recv):
        def one(t, carry):
            to = (r + t) % NR
            pltpu.make_async_remote_copy(
                src_ref=tx.at[to],
                dst_ref=rx.at[r],
                send_sem=send,
                recv_sem=recv,
                device_id=(to, c),
                device_id_type=MESH,
            ).start()
            return carry

        lax.fori_loop(1, NR, one, 0)
        pltpu.make_async_copy(tx.at[r], rx.at[r], recv).start()
        pending[key] = lambda: arrived(rx, recv)
        leaving.append(lambda: arrived(tx.at[pl.ds(0, NR - 1)], send))

    def as_matrix(rx):
        return jnp.concatenate(
            [rx[:, i].astype(F32).reshape(DEPTH, 128) for i in range(OWN)], axis=1
        ).astype(BF16)

    def from_matrix(tx, value):
        for i in range(OWN):
            tx[:, i] = value[:, i * 128 : (i + 1) * 128].reshape(NR, PLACES, 128).astype(BF16)

    def there(layer, s):
        owed(("stats", layer, s))
        totals = jnp.sum(stats_rx[layer, s], axis=0)
        mean = totals[0:2] * (1.0 / 768.0)
        rstd = lax.rsqrt(totals[2:4] * (1.0 / 768.0) - mean * mean + EPS)
        pieces = []
        for hl in range(2):
            value = out[hl, :, s * WIDE : (s + 1) * WIDE]
            normed = ((value - mean[hl : hl + 1]) * rstd[hl : hl + 1]).astype(BF16)
            for pair in range(PAIRS):
                pieces.append(
                    jnp.concatenate(
                        [
                            normed[i * NR : (i + 1) * NR, pair * 128 : (pair + 1) * 128]
                            for i in range(OWN)
                        ],
                        axis=1,
                    )
                )
        tx = there_tx.at[layer, s]
        from_matrix(tx, dot(spread[...], jnp.concatenate(pieces, axis=0)))
        exchange(
            ("there", layer, s), tx, there_rx.at[layer, s], there_s.at[layer, s], there_r.at[layer, s]
        )

    def transform(layer, s):
        owed(("there", layer, s))
        a = dot(fwd_rows[...], as_matrix(there_rx.at[layer, s])).astype(BF16)
        reals, imags = [], []
        for i in range(OWN):
            at = slice(i * 128, (i + 1) * 128)
            b = dot(jnp.concatenate([a[:DEPTH, at], a[DEPTH:, at]], axis=1), fwd_lanes[...])
            b_re = b[:, :128].reshape(PAIRS, GRID, 128)
            b_im = b[:, 128:].reshape(PAIRS, GRID, 128)
            f_re = filt[layer, i, 0:GRID][None]
            f_im = filt[layer, i, GRID:][None]
            c_re = (b_re * f_re - b_im * f_im).reshape(DEPTH, 128)
            c_im = (b_re * f_im + b_im * f_re).reshape(DEPTH, 128)
            e = dot(jnp.concatenate([c_re, c_im], axis=1).astype(BF16), inv_lanes[...]).astype(BF16)
            reals.append(e[:, :128])
            imags.append(e[:, 128:])
        both = jnp.concatenate(
            [jnp.concatenate(reals, axis=1), jnp.concatenate(imags, axis=1)], axis=0
        )
        tx = back_tx.at[layer, s]
        from_matrix(tx, dot(inv_rows[...], both))
        exchange(
            ("back", layer, s), tx, back_rx.at[layer, s], back_s.at[layer, s], back_r.at[layer, s]
        )

    def share(layer, s):
        owed(("back", layer, s))
        mixed = dot(gather[...], as_matrix(back_rx.at[layer, s])).astype(BF16)
        for hl in range(2):
            for pair in range(PAIRS):
                row = (hl * PAIRS + pair) * NR
                for i in range(OWN):
                    ag_tx[layer, s, hl, i * NR : (i + 1) * NR, pair * 128 : (pair + 1) * 128] = mixed[
                        row : row + NR, i * 128 : (i + 1) * 128
                    ]
        own = ag_rx.at[layer, s, c]
        send, recv = ag_s.at[layer, s, 0], ag_r.at[layer, s]
        for way, chip in enumerate((above, below)):
            for k in range(2):
                remote(ag_tx.at[layer, s, k], own, send, recv.at[1 + way], 2 * chip + k)
        remote(ag_tx.at[layer, s, 1 - core], own, send, recv.at[0], 2 * x + 1 - core)
        pltpu.make_async_copy(ag_tx.at[layer, s, core], own, recv.at[0]).start()
        two = ag_rx.at[layer, s, pl.ds(0, 2)]

        def near():
            arrived(two, recv.at[1])
            arrived(two, recv.at[2])

        pending["ag", layer, s] = lambda: arrived(two, recv.at[0])
        pending["near", layer, s] = near
        leaving.append(lambda: arrived(ag_rx.at[layer, s, pl.ds(0, 5)], send))

    def forward(layer, s):
        owed(("near", layer, s))
        send, recv = ag_s.at[layer, s, 1], ag_r.at[layer, s]
        for way, (origin, chip) in enumerate(((below, above), (above, below))):
            ref = ag_rx.at[layer, s, pl.ds(2 * origin, 2), halves[way]]
            remote(ref, ref, send, recv.at[3 + way], 2 * chip + core)

        def further():
            for way in range(2):
                arrived(ag_rx.at[layer, s, pl.ds(2 * across, 2), halves[way]], recv.at[3 + way])

        pending["far", layer, s] = further
        leaving.append(lambda: arrived(ag_rx.at[layer, s, pl.ds(0, 2)], send))

    def mlp(layer, s):
        owed(("ag", layer, s))
        owed(("far", layer, s))
        value = ag_rx[layer, s].astype(F32).reshape(768, WIDE)
        mean = jnp.sum(value, axis=0, keepdims=True) * (1.0 / 768.0)
        square = jnp.sum(value * value, axis=0, keepdims=True) * (1.0 / 768.0)
        rstd = lax.rsqrt(square - mean * mean + EPS)
        normed2 = ((value - mean) * rstd * gcol[layer]).astype(BF16)
        hidden = jax.nn.gelu(dot(et[layer], normed2) + bcol[layer], approximate=True)
        part = dot(st[layer], hidden.astype(BF16))
        rs_tx[layer, s] = part.astype(BF16).reshape(NC, CH, WIDE)
        tx, rx = rs_tx.at[layer, s], rs_rx.at[layer, s]
        send, recv = rs_s.at[layer, s, 0], rs_r.at[layer, s]
        for way, chip in enumerate((above, below)):
            ref = tx.at[pl.ds(2 * across, 2), halves[way]]
            remote(ref, rl_rx.at[layer, s, way], send, recv.at[3 + way], 2 * chip + core)
        for way, chip in enumerate((above, below)):
            for k in range(2):
                remote(
                    tx.at[2 * chip + k, halves[1 - way]],
                    rx.at[1 + way, core, halves[1 - way]],
                    send,
                    recv.at[1 + way],
                    2 * chip + k,
                )
        remote(tx.at[2 * x + 1 - core], rx.at[0, core], send, recv.at[0], 2 * x + 1 - core)
        pltpu.make_async_copy(tx.at[c], rx.at[0, core], recv.at[0]).start()

        def parts():
            for way in range(2):
                arrived(rl_rx.at[layer, s, way], recv.at[3 + way])

        def sums():
            for slot in range(3):
                arrived(rx.at[slot], recv.at[slot])

        pending["rl", layer, s] = parts
        pending["rs", layer, s] = sums
        leaving.append(lambda: arrived(ag_rx.at[layer, s, pl.ds(0, 5)], send))

    def relay(layer, s):
        owed(("rl", layer, s))
        send, recv = rs_s.at[layer, s, 1], rs_r.at[layer, s]
        for way, chip in enumerate((above, below)):
            for k in range(2):
                both = rl_rx[layer, s, way, k].astype(F32) + rs_tx[
                    layer, s, 2 * chip + k, halves[way]
                ].astype(F32)
                rl_tx[layer, s, way, k] = both.astype(BF16)
                remote(
                    rl_tx.at[layer, s, way, k],
                    rs_rx.at[layer, s, 1 + way, core, halves[way]],
                    send,
                    recv.at[1 + way],
                    2 * chip + k,
                )
        leaving.append(lambda: arrived(ag_rx.at[layer, s, pl.ds(0, 2)], send))

    def add(layer, s):
        owed(("rs", layer, s))
        at = slice(s * WIDE, (s + 1) * WIDE)
        for hl in range(2):
            total = rs_rx[layer, s, 0, hl].astype(F32)
            for slot in range(1, 3):
                total = total + rs_rx[layer, s, slot, hl].astype(F32)
            out[hl, :, at] = out[hl, :, at] + total.astype(BF16).astype(F32)
        if layer + 1 < LAYERS:
            send_stats(layer + 1, s)


    plan = [("enter", enter)]

    def then(name, f, *args):
        plan.append((f"{name} {args}", functools.partial(f, *args)))

    def each(name, f, layer):
        for s in range(NS):
            then(name, f, layer, s)

    each("stats", send_stats, 0)
    then("near", hear_near)
    then("wy", wy, 0)
    then("small", send_small)
    then("wy", wy, 1)
    then("far", hear_far)
    then("wz", wz, 0, 1)
    each("there", there, 0)
    then("filters", filters)
    then("columns", columns)
    then("wz", wz, 0, 2)
    each("transform", transform, 0)
    then("wz", wz, 0, 3)
    then("wz", wz, 0, 4)
    each("share", share, 0)
    then("wc", wc, 0)
    then("wz", wz, 1, 1)
    each("forward", forward, 0)
    then("weights", weights, 0)
    each("mlp", mlp, 0)
    each("relay", relay, 0)
    then("wz", wz, 1, 2)
    then("wz", wz, 1, 3)
    each("add", add, 0)
    then("wz", wz, 1, 4)
    each("there", there, 1)
    then("wc", wc, 1)
    each("transform", transform, 1)
    then("weights", weights, 1)
    each("share", share, 1)
    each("forward", forward, 1)
    each("mlp", mlp, 1)
    each("relay", relay, 1)
    each("add", add, 1)

    for _, step in plan[:STOP]:
        step()
    for key in list(pending):
        owed(key)
    for done in leaving:
        done()


def per_device(tokens, spectral, gain_in, gain_mid, expand, bias, shrink):
    hbm = pl.BlockSpec(memory_space=pl.ANY)
    dma = pltpu.SemaphoreType.DMA
    tables = [jnp.asarray(m) for m in matrices()]
    message = (LAYERS, NS, NR, OWN, PLACES, 128)
    scratch = [pltpu.VMEM(m.shape, BF16) for m in tables]
    scratch += [
        pltpu.VMEM((LAYERS, CH), F32),
        pltpu.VMEM((LAYERS, CH), F32),
        pltpu.VMEM((LAYERS, HID), BF16),
        pltpu.VMEM((LAYERS, OWN, GRID, 8, 128), F32),
        pltpu.VMEM((LAYERS, OWN, 128, 128), F32),
        pltpu.VMEM((NC, 4, PIX), F32),
        pltpu.VMEM((LAYERS, NS, NC, 4, WIDE), F32),
        pltpu.VMEM(message, BF16),
        pltpu.VMEM(message, BF16),
        pltpu.VMEM(message, BF16),
        pltpu.VMEM(message, BF16),
        pltpu.VMEM((LAYERS, NS, 2, CH, WIDE), BF16),
        pltpu.VMEM((LAYERS, NS, NC, CH, WIDE), BF16),
        pltpu.VMEM((LAYERS, NS, NC, CH, WIDE), BF16),
        pltpu.VMEM((LAYERS, NS, 3, 2, CH, WIDE), BF16),
        pltpu.VMEM((LAYERS, NS, 2, 2, CH // 2, WIDE), BF16),
        pltpu.VMEM((LAYERS, NS, 2, 2, CH // 2, WIDE), BF16),
        pltpu.VMEM((LAYERS, 2, NZ, NY, 6, 8, HID), BF16),
        pltpu.VMEM((LAYERS, 768, 768), BF16),
        pltpu.VMEM((LAYERS, 768, 768), BF16),
        pltpu.VMEM((LAYERS, 768, 1), F32),
        pltpu.VMEM((LAYERS, 768, 1), F32),
        pltpu.VMEM((128, 128), F32),
        dma((14,)),
        dma((LAYERS, OWN)),
        dma(()),
        dma(()),
    ]
    scratch += [dma((LAYERS, NS))] * 6
    scratch += [dma((LAYERS, NS, 2)), dma((LAYERS, NS, 5))] * 2
    scratch += [dma((LAYERS, NY))] * 2 + [dma((LAYERS, 4, 2))] * 2 + [dma((LAYERS,))] * 2
    scratch += [pltpu.SemaphoreType.REGULAR] * 2
    return pl.pallas_call(
        kernel,
        out_shape=pltpu.VMEM(tokens.shape, F32),
        in_specs=[hbm] * 13,
        out_specs=pl.BlockSpec(memory_space=pltpu.VMEM),
        scratch_shapes=scratch,
        compiler_params=pltpu.CompilerParams(
            collective_id=0, has_side_effects=True, vmem_limit_bytes=56 * 1024 * 1024
        ),
        name="blocks",
    )(
        tokens,
        spectral,
        gain_in,
        gain_mid,
        expand.reshape(LAYERS, 3, 8, HID),
        bias,
        shrink.transpose(0, 2, 1).reshape(LAYERS, 3, 8, HID),
        *tables,
    )


def solution(mesh):
    placed = (
        P("rows", "chan", None),
        P(None, None, "chan", None),
        P(None, "chan"),
        P(None, "chan"),
        P(None, "rows", "chan"),
        P(None, "chan"),
        P(None, "chan", "rows"),
    )
    return jax.shard_map(
        per_device, mesh=mesh, in_specs=placed, out_specs=P("rows", "chan", None), check_vma=False
    )
```

```python
import functools

import jax
import jax.numpy as jnp
import numpy as np
from jax import lax
from jax.experimental import pallas as pl
from jax.experimental.pallas import tpu as pltpu
from jax.sharding import PartitionSpec as P

MESH = pl.DeviceIdType.MESH
F32 = jnp.float32
BF16 = jnp.bfloat16

GRID = 64
LAYERS = 2
NR = 32
NC = 8
NZ, NY = 8, 4
CH = 96
OWN = 3
HID = 384
PIX = 512
NS = 2
WIDE = PIX // NS
PAIRS = WIDE // 128
PLACES = 2 * PAIRS
DEPTH = NR * PLACES
EPS = 1e-06
STOP = None


def matrices():
    index = np.arange(GRID)
    angle = 2.0 * np.pi * ((index[:, None] * index[None, :]) % GRID) / GRID
    cosine, sine = np.cos(angle), np.sin(angle)
    pairs = np.eye(PAIRS)

    def first(table):
        return np.einsum("jh,pq->pjhq", table, pairs).reshape(DEPTH, DEPTH)

    def second(table):
        return np.kron(np.eye(2), table)

    forward_rows = np.concatenate([first(cosine), -first(sine)], axis=0)
    forward_lanes = np.block([[second(cosine), -second(sine)], [second(sine), second(cosine)]])
    inverse_lanes = np.block([[second(cosine), second(sine)], [-second(sine), second(cosine)]])
    inverse_rows = np.concatenate([first(cosine).T, -first(sine).T], axis=1)
    spread = np.zeros((DEPTH, DEPTH))
    for place in range(PLACES):
        for c in range(NR):
            spread[c * PLACES + place, place * NR + c] = 1.0
    return tuple(
        np.asarray(m, dtype=jnp.bfloat16)
        for m in (forward_rows, forward_lanes, inverse_lanes, inverse_rows, spread, spread.T)
    )


def dot(a, b):
    return jnp.dot(a, b, preferred_element_type=F32)


def arrived(ref, sem):
    pltpu.make_async_copy(ref, ref, sem).wait()


def kernel(*refs):
    (
        (tokens, spectral, gain_in, gain_mid, expand, bias, shrink),
        table_hbm,
        (out,),
        table,
        (gi_buf, gm_buf, b_buf, spec_buf, filt, small_rx, stats_rx),
        (there_tx, there_rx, back_tx, back_rx, ag_tx, ag_rx, rs_tx, rs_rx, rl_tx, rl_rx),
        (w_all, et, st, gcol, bcol, turn),
        (in_sem, spec_sem, small_s, small_r, stats_s, stats_r, there_s, there_r, back_s, back_r),
        (ag_s, ag_r, rs_s, rs_r, wy_s, wy_r, wz_s, wz_r, wc_s, wc_r, near_sem, far_sem),
    ) = [
        tuple(refs[a:b])
        for a, b in zip((0, 7, 13, 14, 20, 27, 37, 43, 53), (7, 13, 14, 20, 27, 37, 43, 53, 65))
    ]
    fwd_rows, fwd_lanes, inv_lanes, inv_rows, spread, gather = table

    r = lax.axis_index("rows")
    c = lax.axis_index("chan")
    z, y = r // NY, r % NY
    x, core = c // 2, c % 2
    above, below, across = (x + 1) % 4, (x + 3) % 4, (x + 2) % 4
    halves = (pl.ds(0, CH // 2), pl.ds(CH // 2, CH // 2))

    pending = {}
    leaving = []

    def owed(key):
        pending.pop(key)()

    def remote(src, dst, send, recv, to):
        pltpu.make_async_remote_copy(
            src_ref=src, dst_ref=dst, send_sem=send, recv_sem=recv, device_id=(r, to), device_id_type=MESH
        ).start()


    barrier = pltpu.get_barrier_semaphore()

    def greet_rows(sem, shifts_z, shifts_y=()):
        for t in shifts_z:
            pl.semaphore_signal(
                sem, inc=1, device_id=((z + NZ + t) % NZ * NY + y, c), device_id_type=MESH
            )
        for t in shifts_y:
            pl.semaphore_signal(
                sem, inc=1, device_id=(z * NY + (y + t) % NY, c), device_id_type=MESH
            )

    def greet_chan(t, carry):
        pl.semaphore_signal(barrier, inc=1, device_id=(r, (c + t) % NC), device_id_type=MESH)
        return carry

    def spec_copy(layer, i):
        start = pl.multiple_of(i * NR + r // 8 * 8, 8)
        return pltpu.make_async_copy(
            spectral.at[layer, :, pl.ds(start, 8), :], spec_buf.at[layer, i], spec_sem.at[layer, i]
        )

    loads = [
        (tokens, out),
        (gain_in, gi_buf),
        (gain_mid, gm_buf),
        (bias, b_buf),
        *zip(table_hbm, table),
    ]
    for layer in range(LAYERS):
        own = w_all.at[layer, core, z, y]
        loads.append((expand.at[layer], own.at[pl.ds(0, 3)]))
        loads.append((shrink.at[layer], own.at[pl.ds(3, 3)]))
    loads = [pltpu.make_async_copy(a, b, in_sem.at[k]) for k, (a, b) in enumerate(loads)]

    def put_stats(layer, s):
        at = slice(s * WIDE, (s + 1) * WIDE)
        for hl in range(2):
            value = out[hl, :, at]
            stats_rx[layer, s, c, hl : hl + 1, :] = jnp.sum(value, axis=0, keepdims=True)
            stats_rx[layer, s, c, hl + 2 : hl + 3, :] = jnp.sum(value * value, axis=0, keepdims=True)

    def to_all(key, target, send, recv):
        def one(t, carry):
            to = (c + t) % NC
            pltpu.make_async_remote_copy(
                src_ref=target.at[c],
                dst_ref=target.at[c],
                send_sem=send,
                recv_sem=recv,
                device_id=(r, to),
                device_id_type=MESH,
            ).start()
            return carry

        lax.fori_loop(1, NC, one, 0)
        pending[key] = lambda: arrived(target.at[pl.ds(0, NC - 1)], recv)
        leaving.append(lambda: arrived(target.at[pl.ds(0, NC - 1)], send))

    def send_stats(layer, s):
        put_stats(layer, s)
        buf = stats_rx.at[layer, s]
        to_all(("stats", layer, s), buf, stats_s.at[layer, s], stats_r.at[layer, s])

    def enter():
        lax.fori_loop(1, NC, greet_chan, 0)
        greet_rows(barrier, (-2, -1, 1, 2), (1, 2, 3))
        for copy in loads:
            copy.start()
        for layer in range(LAYERS):
            for i in range(OWN):
                spec_copy(layer, i).start()
                pending["spec", layer, i] = spec_copy(layer, i).wait
        small_rx[c] = jnp.zeros((4, PIX), F32)
        turn[...] = jnp.zeros((128, 128), F32)
        for copy in loads:
            copy.wait()
        small_rx[c, 0:2, 0:CH] = gm_buf[...]
        small_rx[c, 2:4, 0:HID] = b_buf[...].astype(F32)
        pl.semaphore_wait(barrier, NC - 1 + 7)
        greet_rows(near_sem, (-2, -1, 1, 2))


    def hear_near():
        pl.semaphore_wait(near_sem, 4)
        greet_rows(far_sem, (-2, 2))

    def hear_far():
        pl.semaphore_wait(far_sem, 2)

    def send_small():
        to_all("small", small_rx, small_s, small_r)

    def filters():
        lanes = lax.broadcasted_iota(jnp.int32, (1, CH), 1)
        for layer in range(LAYERS):
            for i in range(OWN):
                owed(("spec", layer, i))
                values = spec_buf.at[layer, i].reshape(GRID * 8, 128)[pl.ds(r % 8, GRID, stride=8), :]
                gain = jnp.sum(
                    jnp.where(lanes == i * NR + r, gi_buf[layer : layer + 1, :], 0.0),
                    axis=1,
                    keepdims=True,
                ) * (1.0 / (GRID * GRID))
                values = values * gain
                filt[layer, i] = jnp.concatenate([values, values], axis=0).T

    def columns():
        owed("small")
        for layer in range(LAYERS):
            turn[0:8, :] = small_rx[:, layer, 0:128]
            value = turn[...].T
            for k in range(NC):
                gcol[layer, k * CH : (k + 1) * CH, :] = value[0:CH, k : k + 1]
            for k in range(2):
                for t in range(3):
                    row = 3 * k + t
                    turn[row : row + 1, :] = small_rx[
                        2 * x + k, 2 + layer : 3 + layer, t * 128 : (t + 1) * 128
                    ]
            value = turn[...].T
            for row in range(6):
                bcol[layer, row * 128 : (row + 1) * 128, :] = value[:, row : row + 1]


    def move(ref, send, recv, to, key, expected):
        copy = pltpu.make_async_remote_copy(
            src_ref=ref, dst_ref=ref, send_sem=send, recv_sem=recv, device_id=to, device_id_type=MESH
        )
        copy.start()
        leaving.append(copy.wait_send)
        earlier = pending.get(key)

        def done():
            if earlier is not None:
                earlier()
            arrived(expected, recv)

        pending[key] = done

    def wy(layer):
        ref = w_all.at[layer, core, z, y]
        for t in range(1, NY):
            move(
                ref,
                wy_s.at[layer, t],
                wy_r.at[layer, t],
                (z * NY + (y + t) % NY, c),
                ("w", layer, 0),
                w_all.at[layer, core, z, (y + NY - t) % NY],
            )

    def wz_ref(layer, step, way, shift):
        at = (z + 2 * NZ - shift) % NZ if way == 0 else (z + shift) % NZ
        ref = w_all.at[layer, core, at]
        return ref.at[pl.ds(2 * way, 2)] if step == 4 else ref

    def wz(layer, step):
        if ("w", layer, step - 1) in pending:
            owed(("w", layer, step - 1))
        for way in range(2):
            to = (z + 1) % NZ if way == 0 else (z + NZ - 1) % NZ
            move(
                wz_ref(layer, step, way, step - 1),
                wz_s.at[layer, step - 1, way],
                wz_r.at[layer, step - 1, way],
                (to * NY + y, c),
                ("w", layer, step),
                wz_ref(layer, step, way, step),
            )

    def wc(layer):
        owed(("w", layer, 4))
        move(
            w_all.at[layer, core],
            wc_s.at[layer],
            wc_r.at[layer],
            (r, x * 2 + 1 - core),
            ("w", layer, 5),
            w_all.at[layer, 1 - core],
        )

    def weights(layer):
        owed(("w", layer, 5))
        for k in range(2):
            e = w_all[layer, k, :, :, 0:3].astype(F32).reshape(768, HID)
            et[layer, k * HID : (k + 1) * HID, :] = e.T.astype(BF16)
            s = w_all[layer, k, :, :, 3:6].astype(F32).reshape(768, HID)
            st[layer, :, k * HID : (k + 1) * HID] = s.astype(BF16)


    def exchange(key, tx, rx, send, recv):
        def send_to(to):
            pltpu.make_async_remote_copy(
                src_ref=tx.at[to],
                dst_ref=rx.at[r],
                send_sem=send,
                recv_sem=recv,
                device_id=(to, c),
                device_id_type=MESH,
            ).start()

        def one(t, carry):
            step = (t // NY + 1) // 2 * (t // NY % 2 * 2 - 1)
            send_to((z + NZ // 2 + step + NZ) % NZ * NY + (y + 2 + t) % NY)
            return carry

        lax.fori_loop(0, NR - NY, one, 0)
        for t in range(1, NY):
            send_to(z * NY + (y + t) % NY)
        pltpu.make_async_copy(tx.at[r], rx.at[r], recv).start()
        pending[key] = lambda: arrived(rx, recv)
        leaving.append(lambda: arrived(tx.at[pl.ds(0, NR - 1)], send))

    def as_matrix(rx):
        return jnp.concatenate(
            [rx[:, i].astype(F32).reshape(DEPTH, 128) for i in range(OWN)], axis=1
        ).astype(BF16)

    def from_matrix(tx, value):
        for i in range(OWN):
            tx[:, i] = value[:, i * 128 : (i + 1) * 128].reshape(NR, PLACES, 128).astype(BF16)

    def there(layer, s):
        owed(("stats", layer, s))
        totals = jnp.sum(stats_rx[layer, s], axis=0)
        mean = totals[0:2] * (1.0 / 768.0)
        rstd = lax.rsqrt(totals[2:4] * (1.0 / 768.0) - mean * mean + EPS)
        pieces = []
        for hl in range(2):
            value = out[hl, :, s * WIDE : (s + 1) * WIDE]
            normed = ((value - mean[hl : hl + 1]) * rstd[hl : hl + 1]).astype(BF16)
            for pair in range(PAIRS):
                pieces.append(
                    jnp.concatenate(
                        [
                            normed[i * NR : (i + 1) * NR, pair * 128 : (pair + 1) * 128]
                            for i in range(OWN)
                        ],
                        axis=1,
                    )
                )
        tx = there_tx.at[layer, s]
        from_matrix(tx, dot(spread[...], jnp.concatenate(pieces, axis=0)))
        exchange(
            ("there", layer, s), tx, there_rx.at[layer, s], there_s.at[layer, s], there_r.at[layer, s]
        )

    def transform(layer, s):
        owed(("there", layer, s))
        a = dot(fwd_rows[...], as_matrix(there_rx.at[layer, s])).astype(BF16)
        reals, imags = [], []
        for i in range(OWN):
            at = slice(i * 128, (i + 1) * 128)
            b = dot(jnp.concatenate([a[:DEPTH, at], a[DEPTH:, at]], axis=1), fwd_lanes[...])
            b_re = b[:, :128].reshape(PAIRS, GRID, 128)
            b_im = b[:, 128:].reshape(PAIRS, GRID, 128)
            f_re = filt[layer, i, 0:GRID][None]
            f_im = filt[layer, i, GRID:][None]
            c_re = (b_re * f_re - b_im * f_im).reshape(DEPTH, 128)
            c_im = (b_re * f_im + b_im * f_re).reshape(DEPTH, 128)
            e = dot(jnp.concatenate([c_re, c_im], axis=1).astype(BF16), inv_lanes[...]).astype(BF16)
            reals.append(e[:, :128])
            imags.append(e[:, 128:])
        both = jnp.concatenate(
            [jnp.concatenate(reals, axis=1), jnp.concatenate(imags, axis=1)], axis=0
        )
        tx = back_tx.at[layer, s]
        from_matrix(tx, dot(inv_rows[...], both))
        exchange(
            ("back", layer, s), tx, back_rx.at[layer, s], back_s.at[layer, s], back_r.at[layer, s]
        )

    def share(layer, s):
        owed(("back", layer, s))
        mixed = dot(gather[...], as_matrix(back_rx.at[layer, s])).astype(BF16)
        for hl in range(2):
            for pair in range(PAIRS):
                row = (hl * PAIRS + pair) * NR
                for i in range(OWN):
                    ag_tx[layer, s, hl, i * NR : (i + 1) * NR, pair * 128 : (pair + 1) * 128] = mixed[
                        row : row + NR, i * 128 : (i + 1) * 128
                    ]
        own = ag_rx.at[layer, s, c]
        send, recv = ag_s.at[layer, s], ag_r.at[layer, s]
        for k in range(2):
            remote(ag_tx.at[layer, s, k], own, send, recv.at[3], 2 * across + k)
        for way, chip in enumerate((above, below)):
            for k in range(2):
                remote(ag_tx.at[layer, s, k], own, send, recv.at[1 + way], 2 * chip + k)
        remote(ag_tx.at[layer, s, 1 - core], own, send, recv.at[0], 2 * x + 1 - core)
        pltpu.make_async_copy(ag_tx.at[layer, s, core], own, recv.at[0]).start()
        two = ag_rx.at[layer, s, pl.ds(0, 2)]

        def blocks():
            for k in range(4):
                arrived(two, recv.at[k])

        pending["ag", layer, s] = blocks
        leaving.append(lambda: arrived(ag_rx.at[layer, s, pl.ds(0, 7)], send))

    def mlp(layer, s):
        owed(("ag", layer, s))
        value = ag_rx[layer, s].astype(F32).reshape(768, WIDE)
        mean = jnp.sum(value, axis=0, keepdims=True) * (1.0 / 768.0)
        square = jnp.sum(value * value, axis=0, keepdims=True) * (1.0 / 768.0)
        rstd = lax.rsqrt(square - mean * mean + EPS)
        normed2 = ((value - mean) * rstd * gcol[layer]).astype(BF16)
        hidden = jax.nn.gelu(dot(et[layer], normed2) + bcol[layer], approximate=True)
        part = dot(st[layer], hidden.astype(BF16))
        rs_tx[layer, s] = part.astype(BF16).reshape(NC, CH, WIDE)
        tx, rx = rs_tx.at[layer, s], rs_rx.at[layer, s]
        send, recv = rs_s.at[layer, s, 0], rs_r.at[layer, s]
        for way, chip in enumerate((above, below)):
            ref = tx.at[pl.ds(2 * across, 2), halves[way]]
            remote(ref, rl_rx.at[layer, s, way], send, recv.at[3 + way], 2 * chip + core)
        for way, chip in enumerate((above, below)):
            for k in range(2):
                remote(
                    tx.at[2 * chip + k, halves[1 - way]],
                    rx.at[1 + way, core, halves[1 - way]],
                    send,
                    recv.at[1 + way],
                    2 * chip + k,
                )
        remote(tx.at[2 * x + 1 - core], rx.at[0, core], send, recv.at[0], 2 * x + 1 - core)
        pltpu.make_async_copy(tx.at[c], rx.at[0, core], recv.at[0]).start()

        def parts():
            for way in range(2):
                arrived(rl_rx.at[layer, s, way], recv.at[3 + way])

        def sums():
            for slot in range(3):
                arrived(rx.at[slot], recv.at[slot])

        pending["rl", layer, s] = parts
        pending["rs", layer, s] = sums
        leaving.append(lambda: arrived(ag_rx.at[layer, s, pl.ds(0, 5)], send))

    def relay(layer, s):
        owed(("rl", layer, s))
        send, recv = rs_s.at[layer, s, 1], rs_r.at[layer, s]
        for way, chip in enumerate((above, below)):
            for k in range(2):
                both = rl_rx[layer, s, way, k].astype(F32) + rs_tx[
                    layer, s, 2 * chip + k, halves[way]
                ].astype(F32)
                rl_tx[layer, s, way, k] = both.astype(BF16)
                remote(
                    rl_tx.at[layer, s, way, k],
                    rs_rx.at[layer, s, 1 + way, core, halves[way]],
                    send,
                    recv.at[1 + way],
                    2 * chip + k,
                )
        leaving.append(lambda: arrived(ag_rx.at[layer, s, pl.ds(0, 2)], send))

    def add(layer, s):
        owed(("rs", layer, s))
        at = slice(s * WIDE, (s + 1) * WIDE)
        for hl in range(2):
            total = rs_rx[layer, s, 0, hl].astype(F32)
            for slot in range(1, 3):
                total = total + rs_rx[layer, s, slot, hl].astype(F32)
            out[hl, :, at] = out[hl, :, at] + total.astype(BF16).astype(F32)
        if layer + 1 < LAYERS:
            send_stats(layer + 1, s)


    plan = [("enter", enter)]

    def then(name, f, *args):
        plan.append((f"{name} {args}", functools.partial(f, *args)))

    def each(name, f, layer):
        for s in range(NS):
            then(name, f, layer, s)

    then("wy", wy, 0)
    each("stats", send_stats, 0)
    then("near", hear_near)
    then("wz", wz, 0, 1)
    then("small", send_small)
    then("wy", wy, 1)
    then("far", hear_far)
    each("there", there, 0)
    then("wz", wz, 0, 2)
    then("filters", filters)
    then("columns", columns)
    each("transform", transform, 0)
    then("wz", wz, 0, 3)
    each("share", share, 0)
    then("wz", wz, 0, 4)
    then("wc", wc, 0)
    then("wz", wz, 1, 1)
    then("weights", weights, 0)
    then("wz", wz, 1, 2)
    each("mlp", mlp, 0)
    each("relay", relay, 0)
    then("wz", wz, 1, 3)
    each("add", add, 0)
    each("there", there, 1)
    then("wz", wz, 1, 4)
    each("transform", transform, 1)
    then("wc", wc, 1)
    each("share", share, 1)
    then("weights", weights, 1)
    each("mlp", mlp, 1)
    each("relay", relay, 1)
    each("add", add, 1)

    for _, step in plan[:STOP]:
        step()
    for key in list(pending):
        owed(key)
    for done in leaving:
        done()


def per_device(tokens, spectral, gain_in, gain_mid, expand, bias, shrink):
    hbm = pl.BlockSpec(memory_space=pl.ANY)
    dma = pltpu.SemaphoreType.DMA
    tables = [jnp.asarray(m) for m in matrices()]
    message = (LAYERS, NS, NR, OWN, PLACES, 128)
    scratch = [pltpu.VMEM(m.shape, BF16) for m in tables]
    scratch += [
        pltpu.VMEM((LAYERS, CH), F32),
        pltpu.VMEM((LAYERS, CH), F32),
        pltpu.VMEM((LAYERS, HID), BF16),
        pltpu.VMEM((LAYERS, OWN, GRID, 8, 128), F32),
        pltpu.VMEM((LAYERS, OWN, 128, 128), F32),
        pltpu.VMEM((NC, 4, PIX), F32),
        pltpu.VMEM((LAYERS, NS, NC, 4, WIDE), F32),
        pltpu.VMEM(message, BF16),
        pltpu.VMEM(message, BF16),
        pltpu.VMEM(message, BF16),
        pltpu.VMEM(message, BF16),
        pltpu.VMEM((LAYERS, NS, 2, CH, WIDE), BF16),
        pltpu.VMEM((LAYERS, NS, NC, CH, WIDE), BF16),
        pltpu.VMEM((LAYERS, NS, NC, CH, WIDE), BF16),
        pltpu.VMEM((LAYERS, NS, 3, 2, CH, WIDE), BF16),
        pltpu.VMEM((LAYERS, NS, 2, 2, CH // 2, WIDE), BF16),
        pltpu.VMEM((LAYERS, NS, 2, 2, CH // 2, WIDE), BF16),
        pltpu.VMEM((LAYERS, 2, NZ, NY, 6, 8, HID), BF16),
        pltpu.VMEM((LAYERS, 768, 768), BF16),
        pltpu.VMEM((LAYERS, 768, 768), BF16),
        pltpu.VMEM((LAYERS, 768, 1), F32),
        pltpu.VMEM((LAYERS, 768, 1), F32),
        pltpu.VMEM((128, 128), F32),
        dma((14,)),
        dma((LAYERS, OWN)),
        dma(()),
        dma(()),
    ]
    scratch += [dma((LAYERS, NS))] * 6
    scratch += [dma((LAYERS, NS)), dma((LAYERS, NS, 4))]
    scratch += [dma((LAYERS, NS, 2)), dma((LAYERS, NS, 5))]
    scratch += [dma((LAYERS, NY))] * 2 + [dma((LAYERS, 4, 2))] * 2 + [dma((LAYERS,))] * 2
    scratch += [pltpu.SemaphoreType.REGULAR] * 2
    return pl.pallas_call(
        kernel,
        out_shape=pltpu.VMEM(tokens.shape, F32),
        in_specs=[hbm] * 13,
        out_specs=pl.BlockSpec(memory_space=pltpu.VMEM),
        scratch_shapes=scratch,
        compiler_params=pltpu.CompilerParams(
            collective_id=0, has_side_effects=True, vmem_limit_bytes=56 * 1024 * 1024
        ),
        name="blocks",
    )(
        tokens,
        spectral,
        gain_in,
        gain_mid,
        expand.reshape(LAYERS, 3, 8, HID),
        bias,
        shrink.transpose(0, 2, 1).reshape(LAYERS, 3, 8, HID),
        *tables,
    )


def solution(mesh):
    placed = (
        P("rows", "chan", None),
        P(None, None, "chan", None),
        P(None, "chan"),
        P(None, "chan"),
        P(None, "rows", "chan"),
        P(None, "chan"),
        P(None, "chan", "rows"),
    )
    return jax.shard_map(
        per_device, mesh=mesh, in_specs=placed, out_specs=P("rows", "chan", None), check_vma=False
    )
```

```python
import functools

import jax
import jax.numpy as jnp
import numpy as np
from jax import lax
from jax.experimental import pallas as pl
from jax.experimental.pallas import tpu as pltpu
from jax.sharding import PartitionSpec as P

MESH = pl.DeviceIdType.MESH
F32 = jnp.float32
BF16 = jnp.bfloat16

GRID = 64
LAYERS = 2
NR = 32
NC = 8
NZ, NY = 8, 4
CH = 96
OWN = 3
HID = 384
PIX = 512
NS = 2
WIDE = PIX // NS
PAIRS = WIDE // 128
PLACES = 2 * PAIRS
DEPTH = NR * PLACES
EPS = 1e-06
STOP = None


def matrices():
    index = np.arange(GRID)
    angle = 2.0 * np.pi * ((index[:, None] * index[None, :]) % GRID) / GRID
    cosine, sine = np.cos(angle), np.sin(angle)
    pairs = np.eye(PAIRS)

    def first(table):
        return np.einsum("jh,pq->pjhq", table, pairs).reshape(DEPTH, DEPTH)

    def second(table):
        return np.kron(np.eye(2), table)

    forward_rows = np.concatenate([first(cosine), -first(sine)], axis=0)
    forward_lanes = np.block([[second(cosine), -second(sine)], [second(sine), second(cosine)]])
    inverse_lanes = np.block([[second(cosine), second(sine)], [-second(sine), second(cosine)]])
    inverse_rows = np.concatenate([first(cosine).T, -first(sine).T], axis=1)
    spread = np.zeros((DEPTH, DEPTH))
    for place in range(PLACES):
        for c in range(NR):
            spread[c * PLACES + place, place * NR + c] = 1.0
    return tuple(
        np.asarray(m, dtype=jnp.bfloat16)
        for m in (forward_rows, forward_lanes, inverse_lanes, inverse_rows, spread, spread.T)
    )


def dot(a, b):
    return jnp.dot(a, b, preferred_element_type=F32)


def arrived(ref, sem):
    pltpu.make_async_copy(ref, ref, sem).wait()


def kernel(*refs):
    (
        (tokens, spectral, gain_in, gain_mid, expand, bias, shrink),
        table_hbm,
        (out,),
        table,
        (gi_buf, gm_buf, b_buf, spec_buf, filt, small_rx, stats_rx),
        (there_tx, there_rx, back_tx, back_rx, ag_tx, ag_rx, rs_tx, rs_rx),
        (w_all, et, st, gcol, bcol, turn),
        (in_sem, spec_sem, small_s, small_r, stats_s, stats_r, there_s, there_r, back_s, back_r),
        (ag_s, ag_r, rs_s, rs_r, wy_s, wy_r, wz_s, wz_r, wc_s, wc_r, near_sem, far_sem, wd_r),
    ) = [
        tuple(refs[a:b])
        for a, b in zip((0, 7, 13, 14, 20, 27, 35, 41, 51), (7, 13, 14, 20, 27, 35, 41, 51, 64))
    ]
    fwd_rows, fwd_lanes, inv_lanes, inv_rows, spread, gather = table

    r = lax.axis_index("rows")
    c = lax.axis_index("chan")
    z, y = r // NY, r % NY
    x, core = c // 2, c % 2
    above, below, across = (x + 1) % 4, (x + 3) % 4, (x + 2) % 4

    pending = {}
    leaving = []

    def owed(key):
        pending.pop(key)()

    def remote(src, dst, send, recv, to):
        pltpu.make_async_remote_copy(
            src_ref=src, dst_ref=dst, send_sem=send, recv_sem=recv, device_id=(r, to), device_id_type=MESH
        ).start()


    barrier = pltpu.get_barrier_semaphore()

    def greet_rows(sem, shifts_z, shifts_y=()):
        for t in shifts_z:
            pl.semaphore_signal(
                sem, inc=1, device_id=((z + NZ + t) % NZ * NY + y, c), device_id_type=MESH
            )
        for t in shifts_y:
            pl.semaphore_signal(
                sem, inc=1, device_id=(z * NY + (y + t) % NY, c), device_id_type=MESH
            )

    def greet_chan(t, carry):
        pl.semaphore_signal(barrier, inc=1, device_id=(r, (c + t) % NC), device_id_type=MESH)
        return carry

    def spec_copy(layer, i):
        start = pl.multiple_of(i * NR + r // 8 * 8, 8)
        return pltpu.make_async_copy(
            spectral.at[layer, :, pl.ds(start, 8), :], spec_buf.at[layer, i], spec_sem.at[layer, i]
        )

    loads = [
        (tokens, out),
        (gain_in, gi_buf),
        (gain_mid, gm_buf),
        (bias, b_buf),
        *zip(table_hbm, table),
    ]
    for layer in range(LAYERS):
        own = w_all.at[layer, core, z, y]
        loads.append((expand.at[layer], own.at[pl.ds(0, 3)]))
        loads.append((shrink.at[layer], own.at[pl.ds(3, 3)]))
    loads = [pltpu.make_async_copy(a, b, in_sem.at[k]) for k, (a, b) in enumerate(loads)]

    def put_stats(layer, s):
        at = slice(s * WIDE, (s + 1) * WIDE)
        for hl in range(2):
            value = out[hl, :, at]
            stats_rx[layer, s, c, hl : hl + 1, :] = jnp.sum(value, axis=0, keepdims=True)
            stats_rx[layer, s, c, hl + 2 : hl + 3, :] = jnp.sum(value * value, axis=0, keepdims=True)

    def to_all(key, target, send, recv):
        def one(t, carry):
            to = (c + t) % NC
            pltpu.make_async_remote_copy(
                src_ref=target.at[c],
                dst_ref=target.at[c],
                send_sem=send,
                recv_sem=recv,
                device_id=(r, to),
                device_id_type=MESH,
            ).start()
            return carry

        lax.fori_loop(1, NC, one, 0)
        pending[key] = lambda: arrived(target.at[pl.ds(0, NC - 1)], recv)
        leaving.append(lambda: arrived(target.at[pl.ds(0, NC - 1)], send))

    def send_stats(layer, s):
        put_stats(layer, s)
        buf = stats_rx.at[layer, s]
        to_all(("stats", layer, s), buf, stats_s.at[layer, s], stats_r.at[layer, s])

    def enter():
        lax.fori_loop(1, NC, greet_chan, 0)
        greet_rows(barrier, (-2, -1, 1, 2), (1, 2, 3))
        for copy in loads:
            copy.start()
        for layer in range(LAYERS):
            for i in range(OWN):
                spec_copy(layer, i).start()
                pending["spec", layer, i] = spec_copy(layer, i).wait
        small_rx[c] = jnp.zeros((4, PIX), F32)
        turn[...] = jnp.zeros((128, 128), F32)
        for copy in loads:
            copy.wait()
        small_rx[c, 0:2, 0:CH] = gm_buf[...]
        small_rx[c, 2:4, 0:HID] = b_buf[...].astype(F32)
        pl.semaphore_wait(barrier, NC - 1 + 7)
        greet_rows(near_sem, (-2, -1, 1, 2))


    def hear_near():
        pl.semaphore_wait(near_sem, 4)
        greet_rows(far_sem, (-2, 2))

    def hear_far():
        pl.semaphore_wait(far_sem, 2)

    def send_small():
        to_all("small", small_rx, small_s, small_r)

    def filters():
        lanes = lax.broadcasted_iota(jnp.int32, (1, CH), 1)
        for layer in range(LAYERS):
            for i in range(OWN):
                owed(("spec", layer, i))
                values = spec_buf.at[layer, i].reshape(GRID * 8, 128)[pl.ds(r % 8, GRID, stride=8), :]
                gain = jnp.sum(
                    jnp.where(lanes == i * NR + r, gi_buf[layer : layer + 1, :], 0.0),
                    axis=1,
                    keepdims=True,
                ) * (1.0 / (GRID * GRID))
                values = values * gain
                filt[layer, i] = jnp.concatenate([values, values], axis=0).T

    def columns():
        owed("small")
        for layer in range(LAYERS):
            turn[0:8, :] = small_rx[:, layer, 0:128]
            value = turn[...].T
            for k in range(NC):
                gcol[layer, k * CH : (k + 1) * CH, :] = value[0:CH, k : k + 1]
            for k in range(2):
                for t in range(3):
                    row = 3 * k + t
                    turn[row : row + 1, :] = small_rx[
                        2 * x + k, 2 + layer : 3 + layer, t * 128 : (t + 1) * 128
                    ]
            value = turn[...].T
            for row in range(6):
                bcol[layer, row * 128 : (row + 1) * 128, :] = value[:, row : row + 1]


    def move(ref, send, recv, to, key, expected):
        copy = pltpu.make_async_remote_copy(
            src_ref=ref, dst_ref=ref, send_sem=send, recv_sem=recv, device_id=to, device_id_type=MESH
        )
        copy.start()
        leaving.append(copy.wait_send)
        earlier = pending.get(key)

        def done():
            if earlier is not None:
                earlier()
            arrived(expected, recv)

        pending[key] = done

    def wy(layer):
        ref = w_all.at[layer, core, z, y]
        for t in range(1, NY):
            move(
                ref,
                wy_s.at[layer, t],
                wy_r.at[layer, t],
                (z * NY + (y + t) % NY, c),
                ("w", layer, 0),
                w_all.at[layer, core, z, (y + NY - t) % NY],
            )

    def to_core(layer, parts, last=False):
        for ref in parts:
            pltpu.make_async_remote_copy(
                src_ref=ref,
                dst_ref=ref,
                send_sem=wc_s.at[layer],
                recv_sem=wc_r.at[layer],
                device_id=(r, x * 2 + 1 - core),
                device_id_type=MESH,
            ).start()
        if last:
            pending["w", layer] = lambda: arrived(w_all.at[layer, 1 - core], wc_r.at[layer])
            leaving.append(lambda: arrived(w_all.at[layer, core], wc_s.at[layer]))

    def wz_ref(layer, step, way, shift):
        at = (z + 2 * NZ - shift) % NZ if way == 0 else (z + shift) % NZ
        ref = w_all.at[layer, core, at]
        return ref.at[pl.ds(2 * way, 2)] if step == 4 else ref

    def wz(layer, step):
        owed(("w", layer, step - 1))
        came = (0, 1) if step > 1 else (0,)
        to_core(layer, [wz_ref(layer, 0, way, step - 1) for way in came])
        for way in range(2):
            to = (z + 1) % NZ if way == 0 else (z + NZ - 1) % NZ
            move(
                wz_ref(layer, step, way, step - 1),
                wz_s.at[layer, step - 1, way],
                wz_r.at[layer, step - 1, way],
                (to * NY + y, c),
                ("w", layer, step),
                wz_ref(layer, step, way, step),
            )

    def wc(layer):
        owed(("w", layer, 4))
        to_core(layer, [wz_ref(layer, 0, 0, 4)], last=True)


    near_z, far_z = (0, 1, 2, 6, 7), (3, 4, 5)
    on_way = (((0, 1, 2), (6, 7)), ((3,), (4, 5)))

    def shard(dz, dy):
        return w_all.at[0, core, (z + dz) % NZ, (y + NY + dy) % NY]

    def shards(count):
        return w_all.at[0, core, pl.ds(0, count), 0]

    def wd():
        own = shard(0, 0)
        for t in (1, 7, 2, 6, 3, 5, 4):
            pltpu.make_async_remote_copy(
                src_ref=own,
                dst_ref=own,
                send_sem=wy_s.at[0, 0],
                recv_sem=wd_r.at[NZ - t],
                device_id=((z + t) % NZ * NY + y, c),
                device_id_type=MESH,
            ).start()
            pending["wd", t] = lambda t=t: arrived(shard(t, 0), wd_r.at[t])
        leaving.append(lambda: arrived(shards(NZ - 1), wy_s.at[0, 0]))
        leaving.append(lambda: arrived(w_all.at[0, core, pl.ds(0, 6)], wz_s.at[0, 0, 0]))

    def round_y(ref, way, sem):
        to = (y + 1) % NY if way == 0 else (y + NY - 1) % NY
        pltpu.make_async_remote_copy(
            src_ref=ref,
            dst_ref=ref,
            send_sem=wz_s.at[0, 0, 0],
            recv_sem=sem,
            device_id=(z * NY + to, c),
            device_id_type=MESH,
        ).start()

    def wr(group):
        members = (near_z, far_z)[group]
        for dz in members:
            if dz:
                owed(("wd", dz))
        for way in range(2):
            sem = wz_r.at[0, group, way]
            for dz in members:
                round_y(shard(dz, 0), way, sem)
            pending["wr", group, way] = lambda sem=sem: arrived(shards(len(members)), sem)
        to_core(0, [shard(dz, 0) for dz in members])

    def ws(group):
        members = (near_z, far_z)[group]
        for way in range(2):
            owed(("wr", group, way))
        for way in range(2):
            sem = wz_r.at[0, 2 + group, way]
            chosen = on_way[group][way]
            for dz in chosen:
                round_y(shard(dz, (-1, 1)[way]), way, sem)
            pending["ws", group, way] = lambda sem=sem, n=len(chosen): arrived(shards(n), sem)
        to_core(0, [shard(dz, dy) for dz in members for dy in (-1, 1)])

    def we(group):
        for way in range(2):
            owed(("ws", group, way))
        to_core(0, [shard(dz, 2) for dz in (near_z, far_z)[group]], last=group == 1)

    def weights(layer):
        owed(("w", layer))
        for k in range(2):
            e = w_all[layer, k, :, :, 0:3].astype(F32).reshape(768, HID)
            et[layer, k * HID : (k + 1) * HID, :] = e.T.astype(BF16)
            s = w_all[layer, k, :, :, 3:6].astype(F32).reshape(768, HID)
            st[layer, :, k * HID : (k + 1) * HID] = s.astype(BF16)


    def exchange(key, tx, rx, send, recv):
        def send_to(to):
            pltpu.make_async_remote_copy(
                src_ref=tx.at[to],
                dst_ref=rx.at[r],
                send_sem=send,
                recv_sem=recv,
                device_id=(to, c),
                device_id_type=MESH,
            ).start()

        def one(t, carry):
            step = (t // NY + 1) // 2 * (t // NY % 2 * 2 - 1)
            send_to((z + NZ // 2 + step + NZ) % NZ * NY + (y + 2 + t) % NY)
            return carry

        lax.fori_loop(0, NR - NY, one, 0)
        for t in range(1, NY):
            send_to(z * NY + (y + t) % NY)
        pltpu.make_async_copy(tx.at[r], rx.at[r], recv).start()
        pending[key] = lambda: arrived(rx, recv)
        leaving.append(lambda: arrived(tx.at[pl.ds(0, NR - 1)], send))

    def as_matrix(rx):
        return jnp.concatenate(
            [rx[:, i].astype(F32).reshape(DEPTH, 128) for i in range(OWN)], axis=1
        ).astype(BF16)

    def from_matrix(tx, value):
        for i in range(OWN):
            tx[:, i] = value[:, i * 128 : (i + 1) * 128].reshape(NR, PLACES, 128).astype(BF16)

    def there(layer, s):
        owed(("stats", layer, s))
        totals = jnp.sum(stats_rx[layer, s], axis=0)
        mean = totals[0:2] * (1.0 / 768.0)
        rstd = lax.rsqrt(totals[2:4] * (1.0 / 768.0) - mean * mean + EPS)
        pieces = []
        for hl in range(2):
            value = out[hl, :, s * WIDE : (s + 1) * WIDE]
            normed = ((value - mean[hl : hl + 1]) * rstd[hl : hl + 1]).astype(BF16)
            for pair in range(PAIRS):
                pieces.append(
                    jnp.concatenate(
                        [
                            normed[i * NR : (i + 1) * NR, pair * 128 : (pair + 1) * 128]
                            for i in range(OWN)
                        ],
                        axis=1,
                    )
                )
        tx = there_tx.at[layer, s]
        from_matrix(tx, dot(spread[...], jnp.concatenate(pieces, axis=0)))
        exchange(
            ("there", layer, s), tx, there_rx.at[layer, s], there_s.at[layer, s], there_r.at[layer, s]
        )

    def transform(layer, s):
        owed(("there", layer, s))
        a = dot(fwd_rows[...], as_matrix(there_rx.at[layer, s])).astype(BF16)
        reals, imags = [], []
        for i in range(OWN):
            at = slice(i * 128, (i + 1) * 128)
            b = dot(jnp.concatenate([a[:DEPTH, at], a[DEPTH:, at]], axis=1), fwd_lanes[...])
            b_re = b[:, :128].reshape(PAIRS, GRID, 128)
            b_im = b[:, 128:].reshape(PAIRS, GRID, 128)
            f_re = filt[layer, i, 0:GRID][None]
            f_im = filt[layer, i, GRID:][None]
            c_re = (b_re * f_re - b_im * f_im).reshape(DEPTH, 128)
            c_im = (b_re * f_im + b_im * f_re).reshape(DEPTH, 128)
            e = dot(jnp.concatenate([c_re, c_im], axis=1).astype(BF16), inv_lanes[...]).astype(BF16)
            reals.append(e[:, :128])
            imags.append(e[:, 128:])
        both = jnp.concatenate(
            [jnp.concatenate(reals, axis=1), jnp.concatenate(imags, axis=1)], axis=0
        )
        tx = back_tx.at[layer, s]
        from_matrix(tx, dot(inv_rows[...], both))
        exchange(
            ("back", layer, s), tx, back_rx.at[layer, s], back_s.at[layer, s], back_r.at[layer, s]
        )

    def share(layer, s):
        owed(("back", layer, s))
        mixed = dot(gather[...], as_matrix(back_rx.at[layer, s])).astype(BF16)
        for hl in range(2):
            for pair in range(PAIRS):
                row = (hl * PAIRS + pair) * NR
                for i in range(OWN):
                    ag_tx[layer, s, hl, i * NR : (i + 1) * NR, pair * 128 : (pair + 1) * 128] = mixed[
                        row : row + NR, i * 128 : (i + 1) * 128
                    ]
        own = ag_rx.at[layer, s, c]
        send, recv = ag_s.at[layer, s], ag_r.at[layer, s]
        for k in range(2):
            remote(ag_tx.at[layer, s, k], own, send, recv.at[3], 2 * across + k)
        for way, chip in enumerate((above, below)):
            for k in range(2):
                remote(ag_tx.at[layer, s, k], own, send, recv.at[1 + way], 2 * chip + k)
        remote(ag_tx.at[layer, s, 1 - core], own, send, recv.at[0], 2 * x + 1 - core)
        pltpu.make_async_copy(ag_tx.at[layer, s, core], own, recv.at[0]).start()
        two = ag_rx.at[layer, s, pl.ds(0, 2)]

        def blocks():
            for k in range(4):
                arrived(two, recv.at[k])

        pending["ag", layer, s] = blocks
        leaving.append(lambda: arrived(ag_rx.at[layer, s, pl.ds(0, 7)], send))

    def mlp(layer, s):
        owed(("ag", layer, s))
        value = ag_rx[layer, s].astype(F32).reshape(768, WIDE)
        mean = jnp.sum(value, axis=0, keepdims=True) * (1.0 / 768.0)
        square = jnp.sum(value * value, axis=0, keepdims=True) * (1.0 / 768.0)
        rstd = lax.rsqrt(square - mean * mean + EPS)
        normed2 = ((value - mean) * rstd * gcol[layer]).astype(BF16)
        hidden = jax.nn.gelu(dot(et[layer], normed2) + bcol[layer], approximate=True)
        part = dot(st[layer], hidden.astype(BF16))
        rs_tx[layer, s] = part.astype(BF16).reshape(NC, CH, WIDE)
        tx, rx = rs_tx.at[layer, s], rs_rx.at[layer, s]
        send, recv = rs_s.at[layer, s], rs_r.at[layer, s]
        for slot, chip in ((3, across), (1, above), (2, below)):
            for k in range(2):
                remote(tx.at[2 * chip + k], rx.at[slot, core], send, recv.at[slot], 2 * chip + k)
        remote(tx.at[2 * x + 1 - core], rx.at[0, core], send, recv.at[0], 2 * x + 1 - core)
        pltpu.make_async_copy(tx.at[c], rx.at[0, core], recv.at[0]).start()

        def sums():
            for slot in range(4):
                arrived(rx.at[slot], recv.at[slot])

        pending["rs", layer, s] = sums
        leaving.append(lambda: arrived(ag_rx.at[layer, s, pl.ds(0, 7)], send))

    def add(layer, s):
        owed(("rs", layer, s))
        at = slice(s * WIDE, (s + 1) * WIDE)
        for hl in range(2):
            total = rs_rx[layer, s, 0, hl].astype(F32)
            for slot in range(1, 4):
                total = total + rs_rx[layer, s, slot, hl].astype(F32)
            out[hl, :, at] = out[hl, :, at] + total.astype(BF16).astype(F32)
        if layer + 1 < LAYERS:
            send_stats(layer + 1, s)


    plan = [("enter", enter)]

    def then(name, f, *args):
        plan.append((f"{name} {args}", functools.partial(f, *args)))

    def each(name, f, layer):
        for s in range(NS):
            then(name, f, layer, s)

    each("stats", send_stats, 0)
    then("near", hear_near)
    then("wd", wd)
    then("small", send_small)
    then("wy", wy, 1)
    then("far", hear_far)
    each("there", there, 0)
    then("filters", filters)
    then("columns", columns)
    then("wr", wr, 0)
    then("transform", transform, 0, 0)
    then("wr", wr, 1)
    then("transform", transform, 0, 1)
    then("ws", ws, 0)
    then("ws", ws, 1)
    then("we", we, 0)
    each("share", share, 0)
    then("we", we, 1)
    then("wz", wz, 1, 1)
    then("weights", weights, 0)
    then("wz", wz, 1, 2)
    each("mlp", mlp, 0)
    then("wz", wz, 1, 3)
    each("add", add, 0)
    each("there", there, 1)
    then("wz", wz, 1, 4)
    each("transform", transform, 1)
    then("wc", wc, 1)
    each("share", share, 1)
    then("weights", weights, 1)
    each("mlp", mlp, 1)
    each("add", add, 1)

    for _, step in plan[:STOP]:
        step()
    for key in list(pending):
        owed(key)
    for done in leaving:
        done()


def per_device(tokens, spectral, gain_in, gain_mid, expand, bias, shrink):
    hbm = pl.BlockSpec(memory_space=pl.ANY)
    dma = pltpu.SemaphoreType.DMA
    tables = [jnp.asarray(m) for m in matrices()]
    message = (LAYERS, NS, NR, OWN, PLACES, 128)
    scratch = [pltpu.VMEM(m.shape, BF16) for m in tables]
    scratch += [
        pltpu.VMEM((LAYERS, CH), F32),
        pltpu.VMEM((LAYERS, CH), F32),
        pltpu.VMEM((LAYERS, HID), BF16),
        pltpu.VMEM((LAYERS, OWN, GRID, 8, 128), F32),
        pltpu.VMEM((LAYERS, OWN, 128, 128), F32),
        pltpu.VMEM((NC, 4, PIX), F32),
        pltpu.VMEM((LAYERS, NS, NC, 4, WIDE), F32),
        pltpu.VMEM(message, BF16),
        pltpu.VMEM(message, BF16),
        pltpu.VMEM(message, BF16),
        pltpu.VMEM(message, BF16),
        pltpu.VMEM((LAYERS, NS, 2, CH, WIDE), BF16),
        pltpu.VMEM((LAYERS, NS, NC, CH, WIDE), BF16),
        pltpu.VMEM((LAYERS, NS, NC, CH, WIDE), BF16),
        pltpu.VMEM((LAYERS, NS, 4, 2, CH, WIDE), BF16),
        pltpu.VMEM((LAYERS, 2, NZ, NY, 6, 8, HID), BF16),
        pltpu.VMEM((LAYERS, 768, 768), BF16),
        pltpu.VMEM((LAYERS, 768, 768), BF16),
        pltpu.VMEM((LAYERS, 768, 1), F32),
        pltpu.VMEM((LAYERS, 768, 1), F32),
        pltpu.VMEM((128, 128), F32),
        dma((14,)),
        dma((LAYERS, OWN)),
        dma(()),
        dma(()),
    ]
    scratch += [dma((LAYERS, NS))] * 6
    scratch += [dma((LAYERS, NS)), dma((LAYERS, NS, 4))]
    scratch += [dma((LAYERS, NS)), dma((LAYERS, NS, 4))]
    scratch += [dma((LAYERS, NY))] * 2 + [dma((LAYERS, 4, 2))] * 2 + [dma((LAYERS,))] * 2
    scratch += [pltpu.SemaphoreType.REGULAR] * 2 + [dma((NZ,))]
    return pl.pallas_call(
        kernel,
        out_shape=pltpu.VMEM(tokens.shape, F32),
        in_specs=[hbm] * 13,
        out_specs=pl.BlockSpec(memory_space=pltpu.VMEM),
        scratch_shapes=scratch,
        compiler_params=pltpu.CompilerParams(
            collective_id=0, has_side_effects=True, vmem_limit_bytes=56 * 1024 * 1024
        ),
        name="blocks",
    )(
        tokens,
        spectral,
        gain_in,
        gain_mid,
        expand.reshape(LAYERS, 3, 8, HID),
        bias,
        shrink.transpose(0, 2, 1).reshape(LAYERS, 3, 8, HID),
        *tables,
    )


def solution(mesh):
    placed = (
        P("rows", "chan", None),
        P(None, None, "chan", None),
        P(None, "chan"),
        P(None, "chan"),
        P(None, "rows", "chan"),
        P(None, "chan"),
        P(None, "chan", "rows"),
    )
    return jax.shard_map(
        per_device, mesh=mesh, in_specs=placed, out_specs=P("rows", "chan", None), check_vma=False
    )
```

```python
import functools

import jax
import jax.numpy as jnp
import numpy as np
from jax import lax
from jax.experimental import pallas as pl
from jax.experimental.pallas import tpu as pltpu
from jax.sharding import PartitionSpec as P

MESH = pl.DeviceIdType.MESH
F32 = jnp.float32
BF16 = jnp.bfloat16

GRID = 64
LAYERS = 2
NR = 32
NC = 8
NZ, NY = 8, 4
CH = 96
OWN = 3
HID = 384
PIX = 512
NS = 2
WIDE = PIX // NS
PAIRS = WIDE // 128
PLACES = 2 * PAIRS
DEPTH = NR * PLACES
EPS = 1e-06
STOP = None


def matrices():
    index = np.arange(GRID)
    angle = 2.0 * np.pi * ((index[:, None] * index[None, :]) % GRID) / GRID
    cosine, sine = np.cos(angle), np.sin(angle)
    pairs = np.eye(PAIRS)

    def first(table):
        return np.einsum("jh,pq->pjhq", table, pairs).reshape(DEPTH, DEPTH)

    def second(table):
        return np.kron(np.eye(2), table)

    forward_rows = np.concatenate([first(cosine), -first(sine)], axis=0)
    forward_lanes = np.block([[second(cosine), -second(sine)], [second(sine), second(cosine)]])
    inverse_lanes = np.block([[second(cosine), second(sine)], [-second(sine), second(cosine)]])
    inverse_rows = np.concatenate([first(cosine).T, -first(sine).T], axis=1)
    spread = np.zeros((DEPTH, DEPTH))
    for place in range(PLACES):
        for c in range(NR):
            spread[c * PLACES + place, place * NR + c] = 1.0
    return tuple(
        np.asarray(m, dtype=jnp.bfloat16)
        for m in (forward_rows, forward_lanes, inverse_lanes, inverse_rows, spread, spread.T)
    )


def dot(a, b):
    return jnp.dot(a, b, preferred_element_type=F32)


def arrived(ref, sem):
    pltpu.make_async_copy(ref, ref, sem).wait()


def kernel(*refs):
    (
        (tokens, spectral, gain_in, gain_mid, expand, bias, shrink),
        table_hbm,
        (out,),
        table,
        (gi_buf, gm_buf, b_buf, spec_buf, filt, small_rx, stats_rx),
        (there_tx, there_rx, back_tx, back_rx, ag_tx, ag_rx, rs_tx, rs_rx),
        (w_all, et, st, gcol, bcol, turn),
        (in_sem, spec_sem, small_s, small_r, stats_s, stats_r, there_s, there_r, back_s, back_r),
        (ag_s, ag_r, rs_s, rs_r, wy_s, wy_r, wz_s, wz_r, wc_s, wc_r, near_sem, far_sem, wd_r),
    ) = [
        tuple(refs[a:b])
        for a, b in zip((0, 7, 13, 14, 20, 27, 35, 41, 51), (7, 13, 14, 20, 27, 35, 41, 51, 64))
    ]
    fwd_rows, fwd_lanes, inv_lanes, inv_rows, spread, gather = table

    r = lax.axis_index("rows")
    c = lax.axis_index("chan")
    z, y = r // NY, r % NY
    x, core = c // 2, c % 2
    above, below, across = (x + 1) % 4, (x + 3) % 4, (x + 2) % 4

    pending = {}
    leaving = []

    def owed(key):
        pending.pop(key)()

    def remote(src, dst, send, recv, to):
        pltpu.make_async_remote_copy(
            src_ref=src, dst_ref=dst, send_sem=send, recv_sem=recv, device_id=(r, to), device_id_type=MESH
        ).start()


    barrier = pltpu.get_barrier_semaphore()

    def greet_rows(sem, shifts_z, shifts_y=()):
        for t in shifts_z:
            pl.semaphore_signal(
                sem, inc=1, device_id=((z + NZ + t) % NZ * NY + y, c), device_id_type=MESH
            )
        for t in shifts_y:
            pl.semaphore_signal(
                sem, inc=1, device_id=(z * NY + (y + t) % NY, c), device_id_type=MESH
            )

    def greet_chan(t, carry):
        pl.semaphore_signal(barrier, inc=1, device_id=(r, (c + t) % NC), device_id_type=MESH)
        return carry

    def spec_copy(layer, i):
        start = pl.multiple_of(i * NR + r // 8 * 8, 8)
        return pltpu.make_async_copy(
            spectral.at[layer, :, pl.ds(start, 8), :], spec_buf.at[layer, i], spec_sem.at[layer, i]
        )

    loads = [
        (tokens, out),
        (gain_in, gi_buf),
        (gain_mid, gm_buf),
        (bias, b_buf),
        *zip(table_hbm, table),
    ]
    for layer in range(LAYERS):
        own = w_all.at[layer, core, z, y]
        loads.append((expand.at[layer], own.at[pl.ds(0, 3)]))
        loads.append((shrink.at[layer], own.at[pl.ds(3, 3)]))
    loads = [pltpu.make_async_copy(a, b, in_sem.at[k]) for k, (a, b) in enumerate(loads)]

    def put_stats(layer, s):
        at = slice(s * WIDE, (s + 1) * WIDE)
        for hl in range(2):
            value = out[hl, :, at]
            stats_rx[layer, s, c, hl : hl + 1, :] = jnp.sum(value, axis=0, keepdims=True)
            stats_rx[layer, s, c, hl + 2 : hl + 3, :] = jnp.sum(value * value, axis=0, keepdims=True)

    def to_all(key, target, send, recv):
        def one(t, carry):
            to = (c + t) % NC
            pltpu.make_async_remote_copy(
                src_ref=target.at[c],
                dst_ref=target.at[c],
                send_sem=send,
                recv_sem=recv,
                device_id=(r, to),
                device_id_type=MESH,
            ).start()
            return carry

        lax.fori_loop(1, NC, one, 0)
        pending[key] = lambda: arrived(target.at[pl.ds(0, NC - 1)], recv)
        leaving.append(lambda: arrived(target.at[pl.ds(0, NC - 1)], send))

    def send_stats(layer, s):
        if layer:
            put_stats(layer, s)
        buf = stats_rx.at[layer, s]
        to_all(("stats", layer, s), buf, stats_s.at[layer, s], stats_r.at[layer, s])

    def enter():
        lax.fori_loop(1, NC, greet_chan, 0)
        greet_rows(barrier, (-2, -1, 1, 2), (1, 2, 3))
        for copy in loads:
            copy.start()
        for layer in range(LAYERS):
            for i in range(OWN):
                spec_copy(layer, i).start()
                pending["spec", layer, i] = spec_copy(layer, i).wait
        small_rx[c] = jnp.zeros((4, PIX), F32)
        turn[...] = jnp.zeros((128, 128), F32)
        loads[0].wait()
        for s in range(NS):
            put_stats(0, s)
        for copy in loads[1:]:
            copy.wait()
        small_rx[c, 0:2, 0:CH] = gm_buf[...]
        small_rx[c, 2:4, 0:HID] = b_buf[...].astype(F32)
        pl.semaphore_wait(barrier, NC - 1 + 7)
        greet_rows(near_sem, (-2, -1, 1, 2))


    def hear_near():
        pl.semaphore_wait(near_sem, 4)
        greet_rows(far_sem, (-2, 2))

    def hear_far():
        pl.semaphore_wait(far_sem, 2)

    def send_small():
        to_all("small", small_rx, small_s, small_r)

    def filters():
        lanes = lax.broadcasted_iota(jnp.int32, (1, CH), 1)
        for layer in range(LAYERS):
            for i in range(OWN):
                owed(("spec", layer, i))
                values = spec_buf.at[layer, i].reshape(GRID * 8, 128)[pl.ds(r % 8, GRID, stride=8), :]
                gain = jnp.sum(
                    jnp.where(lanes == i * NR + r, gi_buf[layer : layer + 1, :], 0.0),
                    axis=1,
                    keepdims=True,
                ) * (1.0 / (GRID * GRID))
                values = values * gain
                filt[layer, i] = jnp.concatenate([values, values], axis=0).T

    def columns():
        owed("small")
        for layer in range(LAYERS):
            turn[0:8, :] = small_rx[:, layer, 0:128]
            value = turn[...].T
            for k in range(NC):
                gcol[layer, k * CH : (k + 1) * CH, :] = value[0:CH, k : k + 1]
            for k in range(2):
                for t in range(3):
                    row = 3 * k + t
                    turn[row : row + 1, :] = small_rx[
                        2 * x + k, 2 + layer : 3 + layer, t * 128 : (t + 1) * 128
                    ]
            value = turn[...].T
            for row in range(6):
                bcol[layer, row * 128 : (row + 1) * 128, :] = value[:, row : row + 1]


    def move(ref, send, recv, to, key, expected):
        copy = pltpu.make_async_remote_copy(
            src_ref=ref, dst_ref=ref, send_sem=send, recv_sem=recv, device_id=to, device_id_type=MESH
        )
        copy.start()
        leaving.append(copy.wait_send)
        earlier = pending.get(key)

        def done():
            if earlier is not None:
                earlier()
            arrived(expected, recv)

        pending[key] = done

    def wy(layer):
        ref = w_all.at[layer, core, z, y]
        for t in range(1, NY):
            move(
                ref,
                wy_s.at[layer, t],
                wy_r.at[layer, t],
                (z * NY + (y + t) % NY, c),
                ("w", layer, 0),
                w_all.at[layer, core, z, (y + NY - t) % NY],
            )

    def to_core(layer, parts, last=False):
        for ref in parts:
            pltpu.make_async_remote_copy(
                src_ref=ref,
                dst_ref=ref,
                send_sem=wc_s.at[layer],
                recv_sem=wc_r.at[layer],
                device_id=(r, x * 2 + 1 - core),
                device_id_type=MESH,
            ).start()
        if last:
            pending["w", layer] = lambda: arrived(w_all.at[layer, 1 - core], wc_r.at[layer])
            leaving.append(lambda: arrived(w_all.at[layer, core], wc_s.at[layer]))

    def wz_ref(layer, step, way, shift):
        at = (z + 2 * NZ - shift) % NZ if way == 0 else (z + shift) % NZ
        ref = w_all.at[layer, core, at]
        return ref.at[pl.ds(2 * way, 2)] if step == 4 else ref

    def wz(layer, step):
        owed(("w", layer, step - 1))
        came = (0, 1) if step > 1 else (0,)
        to_core(layer, [wz_ref(layer, 0, way, step - 1) for way in came])
        for way in range(2):
            to = (z + 1) % NZ if way == 0 else (z + NZ - 1) % NZ
            move(
                wz_ref(layer, step, way, step - 1),
                wz_s.at[layer, step - 1, way],
                wz_r.at[layer, step - 1, way],
                (to * NY + y, c),
                ("w", layer, step),
                wz_ref(layer, step, way, step),
            )

    def wc(layer):
        owed(("w", layer, 4))
        to_core(layer, [wz_ref(layer, 0, 0, 4)], last=True)


    near_z, far_z = (0, 1, 2, 6, 7), (3, 4, 5)
    on_way = (((0, 1, 2), (6, 7)), ((3,), (4, 5)))

    def shard(dz, dy):
        return w_all.at[0, core, (z + dz) % NZ, (y + NY + dy) % NY]

    def shards(count):
        return w_all.at[0, core, pl.ds(0, count), 0]

    def along_z(ref, t, dz):
        pltpu.make_async_remote_copy(
            src_ref=ref,
            dst_ref=ref,
            send_sem=wy_s.at[0, 0],
            recv_sem=wd_r.at[dz],
            device_id=((z + t) % NZ * NY + y, c),
            device_id_type=MESH,
        ).start()
        pending["wd", dz] = lambda: arrived(shard(dz, 0), wd_r.at[dz])

    def wd():
        for t in (2, 6, 1, 7):
            along_z(shard(0, 0), t, NZ - t)
        leaving.append(lambda: arrived(shards(NZ - 1), wy_s.at[0, 0]))
        leaving.append(lambda: arrived(w_all.at[0, core, pl.ds(0, 6)], wz_s.at[0, 0, 0]))

    def wf():
        owed(("wd", 2))
        owed(("wd", 6))
        along_z(shard(6, 0), 2, 4)
        along_z(shard(6, 0), 1, 5)
        along_z(shard(2, 0), 7, 3)

    def round_y(ref, way, sem):
        to = (y + 1) % NY if way == 0 else (y + NY - 1) % NY
        pltpu.make_async_remote_copy(
            src_ref=ref,
            dst_ref=ref,
            send_sem=wz_s.at[0, 0, 0],
            recv_sem=sem,
            device_id=(z * NY + to, c),
            device_id_type=MESH,
        ).start()

    def wr(group):
        members = (near_z, far_z)[group]
        for dz in members:
            if ("wd", dz) in pending:
                owed(("wd", dz))
        for way in range(2):
            sem = wz_r.at[0, group, way]
            for dz in members:
                round_y(shard(dz, 0), way, sem)
            pending["wr", group, way] = lambda sem=sem: arrived(shards(len(members)), sem)
        to_core(0, [shard(dz, 0) for dz in members])

    def ws(group):
        members = (near_z, far_z)[group]
        for way in range(2):
            owed(("wr", group, way))
        for way in range(2):
            sem = wz_r.at[0, 2 + group, way]
            chosen = on_way[group][way]
            for dz in chosen:
                round_y(shard(dz, (-1, 1)[way]), way, sem)
            pending["ws", group, way] = lambda sem=sem, n=len(chosen): arrived(shards(n), sem)
        to_core(0, [shard(dz, dy) for dz in members for dy in (-1, 1)])

    def we(group):
        for way in range(2):
            owed(("ws", group, way))
        to_core(0, [shard(dz, 2) for dz in (near_z, far_z)[group]], last=group == 1)

    def weights(layer):
        owed(("w", layer))
        for k in range(2):
            e = w_all[layer, k, :, :, 0:3].astype(F32).reshape(768, HID)
            et[layer, k * HID : (k + 1) * HID, :] = e.T.astype(BF16)
            s = w_all[layer, k, :, :, 3:6].astype(F32).reshape(768, HID)
            st[layer, :, k * HID : (k + 1) * HID] = s.astype(BF16)


    def exchange(key, tx, rx, send, recv):
        def send_to(to):
            pltpu.make_async_remote_copy(
                src_ref=tx.at[to],
                dst_ref=rx.at[r],
                send_sem=send,
                recv_sem=recv,
                device_id=(to, c),
                device_id_type=MESH,
            ).start()

        def one(t, carry):
            step = (t // NY + 1) // 2 * (t // NY % 2 * 2 - 1)
            send_to((z + NZ // 2 + step + NZ) % NZ * NY + (y + 2 + t) % NY)
            return carry

        lax.fori_loop(0, NR - NY, one, 0)
        for t in range(1, NY):
            send_to(z * NY + (y + t) % NY)
        pltpu.make_async_copy(tx.at[r], rx.at[r], recv).start()
        pending[key] = lambda: arrived(rx, recv)
        leaving.append(lambda: arrived(tx.at[pl.ds(0, NR - 1)], send))

    def as_matrix(rx):
        return jnp.concatenate(
            [rx[:, i].astype(F32).reshape(DEPTH, 128) for i in range(OWN)], axis=1
        ).astype(BF16)

    def from_matrix(tx, value):
        for i in range(OWN):
            tx[:, i] = value[:, i * 128 : (i + 1) * 128].reshape(NR, PLACES, 128).astype(BF16)

    def there(layer, s):
        owed(("stats", layer, s))
        totals = jnp.sum(stats_rx[layer, s], axis=0)
        mean = totals[0:2] * (1.0 / 768.0)
        rstd = lax.rsqrt(totals[2:4] * (1.0 / 768.0) - mean * mean + EPS)
        pieces = []
        for hl in range(2):
            value = out[hl, :, s * WIDE : (s + 1) * WIDE]
            normed = ((value - mean[hl : hl + 1]) * rstd[hl : hl + 1]).astype(BF16)
            for pair in range(PAIRS):
                pieces.append(
                    jnp.concatenate(
                        [
                            normed[i * NR : (i + 1) * NR, pair * 128 : (pair + 1) * 128]
                            for i in range(OWN)
                        ],
                        axis=1,
                    )
                )
        tx = there_tx.at[layer, s]
        from_matrix(tx, dot(spread[...], jnp.concatenate(pieces, axis=0)))
        exchange(
            ("there", layer, s), tx, there_rx.at[layer, s], there_s.at[layer, s], there_r.at[layer, s]
        )

    def transform(layer, s):
        owed(("there", layer, s))
        a = dot(fwd_rows[...], as_matrix(there_rx.at[layer, s])).astype(BF16)
        reals, imags = [], []
        for i in range(OWN):
            at = slice(i * 128, (i + 1) * 128)
            b = dot(jnp.concatenate([a[:DEPTH, at], a[DEPTH:, at]], axis=1), fwd_lanes[...])
            b_re = b[:, :128].reshape(PAIRS, GRID, 128)
            b_im = b[:, 128:].reshape(PAIRS, GRID, 128)
            f_re = filt[layer, i, 0:GRID][None]
            f_im = filt[layer, i, GRID:][None]
            c_re = (b_re * f_re - b_im * f_im).reshape(DEPTH, 128)
            c_im = (b_re * f_im + b_im * f_re).reshape(DEPTH, 128)
            e = dot(jnp.concatenate([c_re, c_im], axis=1).astype(BF16), inv_lanes[...]).astype(BF16)
            reals.append(e[:, :128])
            imags.append(e[:, 128:])
        both = jnp.concatenate(
            [jnp.concatenate(reals, axis=1), jnp.concatenate(imags, axis=1)], axis=0
        )
        tx = back_tx.at[layer, s]
        from_matrix(tx, dot(inv_rows[...], both))
        exchange(
            ("back", layer, s), tx, back_rx.at[layer, s], back_s.at[layer, s], back_r.at[layer, s]
        )

    def share(layer, s):
        owed(("back", layer, s))
        mixed = dot(gather[...], as_matrix(back_rx.at[layer, s])).astype(BF16)
        for hl in range(2):
            for pair in range(PAIRS):
                row = (hl * PAIRS + pair) * NR
                for i in range(OWN):
                    ag_tx[layer, s, hl, i * NR : (i + 1) * NR, pair * 128 : (pair + 1) * 128] = mixed[
                        row : row + NR, i * 128 : (i + 1) * 128
                    ]
        own = ag_rx.at[layer, s, c]
        send, recv = ag_s.at[layer, s], ag_r.at[layer, s]
        for k in range(2):
            remote(ag_tx.at[layer, s, k], own, send, recv.at[3], 2 * across + k)
        for way, chip in enumerate((above, below)):
            for k in range(2):
                remote(ag_tx.at[layer, s, k], own, send, recv.at[1 + way], 2 * chip + k)
        remote(ag_tx.at[layer, s, 1 - core], own, send, recv.at[0], 2 * x + 1 - core)
        pltpu.make_async_copy(ag_tx.at[layer, s, core], own, recv.at[0]).start()
        two = ag_rx.at[layer, s, pl.ds(0, 2)]

        def blocks():
            for k in range(4):
                arrived(two, recv.at[k])

        pending["ag", layer, s] = blocks
        leaving.append(lambda: arrived(ag_rx.at[layer, s, pl.ds(0, 7)], send))

    def mlp(layer, s):
        owed(("ag", layer, s))
        value = ag_rx[layer, s].astype(F32).reshape(768, WIDE)
        mean = jnp.sum(value, axis=0, keepdims=True) * (1.0 / 768.0)
        square = jnp.sum(value * value, axis=0, keepdims=True) * (1.0 / 768.0)
        rstd = lax.rsqrt(square - mean * mean + EPS)
        normed2 = ((value - mean) * rstd * gcol[layer]).astype(BF16)
        hidden = jax.nn.gelu(dot(et[layer], normed2) + bcol[layer], approximate=True)
        part = dot(st[layer], hidden.astype(BF16))
        rs_tx[layer, s] = part.astype(BF16).reshape(NC, CH, WIDE)
        tx, rx = rs_tx.at[layer, s], rs_rx.at[layer, s]
        send, recv = rs_s.at[layer, s], rs_r.at[layer, s]
        for slot, chip in ((3, across), (1, above), (2, below)):
            for k in range(2):
                remote(tx.at[2 * chip + k], rx.at[slot, core], send, recv.at[slot], 2 * chip + k)
        remote(tx.at[2 * x + 1 - core], rx.at[0, core], send, recv.at[0], 2 * x + 1 - core)
        pltpu.make_async_copy(tx.at[c], rx.at[0, core], recv.at[0]).start()

        def sums():
            for slot in range(4):
                arrived(rx.at[slot], recv.at[slot])

        pending["rs", layer, s] = sums
        leaving.append(lambda: arrived(ag_rx.at[layer, s, pl.ds(0, 7)], send))

    def add(layer, s):
        owed(("rs", layer, s))
        at = slice(s * WIDE, (s + 1) * WIDE)
        for hl in range(2):
            total = rs_rx[layer, s, 0, hl].astype(F32)
            for slot in range(1, 4):
                total = total + rs_rx[layer, s, slot, hl].astype(F32)
            out[hl, :, at] = out[hl, :, at] + total.astype(BF16).astype(F32)
        if layer + 1 < LAYERS:
            send_stats(layer + 1, s)


    plan = [("enter", enter)]

    def then(name, f, *args):
        plan.append((f"{name} {args}", functools.partial(f, *args)))

    def each(name, f, layer):
        for s in range(NS):
            then(name, f, layer, s)

    each("stats", send_stats, 0)
    then("near", hear_near)
    then("wd", wd)
    then("small", send_small)
    then("wy", wy, 1)
    then("far", hear_far)
    each("there", there, 0)
    then("wf", wf)
    then("wr", wr, 0)
    then("filters", filters)
    then("columns", columns)
    then("transform", transform, 0, 0)
    then("wr", wr, 1)
    then("transform", transform, 0, 1)
    then("ws", ws, 0)
    then("ws", ws, 1)
    then("we", we, 0)
    each("share", share, 0)
    then("we", we, 1)
    then("wz", wz, 1, 1)
    then("weights", weights, 0)
    then("wz", wz, 1, 2)
    each("mlp", mlp, 0)
    then("wz", wz, 1, 3)
    each("add", add, 0)
    each("there", there, 1)
    then("wz", wz, 1, 4)
    each("transform", transform, 1)
    then("wc", wc, 1)
    each("share", share, 1)
    then("weights", weights, 1)
    each("mlp", mlp, 1)
    each("add", add, 1)

    for _, step in plan[:STOP]:
        step()
    for key in list(pending):
        owed(key)
    for done in leaving:
        done()


def per_device(tokens, spectral, gain_in, gain_mid, expand, bias, shrink):
    hbm = pl.BlockSpec(memory_space=pl.ANY)
    dma = pltpu.SemaphoreType.DMA
    tables = [jnp.asarray(m) for m in matrices()]
    message = (LAYERS, NS, NR, OWN, PLACES, 128)
    scratch = [pltpu.VMEM(m.shape, BF16) for m in tables]
    scratch += [
        pltpu.VMEM((LAYERS, CH), F32),
        pltpu.VMEM((LAYERS, CH), F32),
        pltpu.VMEM((LAYERS, HID), BF16),
        pltpu.VMEM((LAYERS, OWN, GRID, 8, 128), F32),
        pltpu.VMEM((LAYERS, OWN, 128, 128), F32),
        pltpu.VMEM((NC, 4, PIX), F32),
        pltpu.VMEM((LAYERS, NS, NC, 4, WIDE), F32),
        pltpu.VMEM(message, BF16),
        pltpu.VMEM(message, BF16),
        pltpu.VMEM(message, BF16),
        pltpu.VMEM(message, BF16),
        pltpu.VMEM((LAYERS, NS, 2, CH, WIDE), BF16),
        pltpu.VMEM((LAYERS, NS, NC, CH, WIDE), BF16),
        pltpu.VMEM((LAYERS, NS, NC, CH, WIDE), BF16),
        pltpu.VMEM((LAYERS, NS, 4, 2, CH, WIDE), BF16),
        pltpu.VMEM((LAYERS, 2, NZ, NY, 6, 8, HID), BF16),
        pltpu.VMEM((LAYERS, 768, 768), BF16),
        pltpu.VMEM((LAYERS, 768, 768), BF16),
        pltpu.VMEM((LAYERS, 768, 1), F32),
        pltpu.VMEM((LAYERS, 768, 1), F32),
        pltpu.VMEM((128, 128), F32),
        dma((14,)),
        dma((LAYERS, OWN)),
        dma(()),
        dma(()),
    ]
    scratch += [dma((LAYERS, NS))] * 6
    scratch += [dma((LAYERS, NS)), dma((LAYERS, NS, 4))]
    scratch += [dma((LAYERS, NS)), dma((LAYERS, NS, 4))]
    scratch += [dma((LAYERS, NY))] * 2 + [dma((LAYERS, 4, 2))] * 2 + [dma((LAYERS,))] * 2
    scratch += [pltpu.SemaphoreType.REGULAR] * 2 + [dma((NZ,))]
    return pl.pallas_call(
        kernel,
        out_shape=pltpu.VMEM(tokens.shape, F32),
        in_specs=[hbm] * 13,
        out_specs=pl.BlockSpec(memory_space=pltpu.VMEM),
        scratch_shapes=scratch,
        compiler_params=pltpu.CompilerParams(
            collective_id=0, has_side_effects=True, vmem_limit_bytes=56 * 1024 * 1024
        ),
        name="blocks",
    )(
        tokens,
        spectral,
        gain_in,
        gain_mid,
        expand.reshape(LAYERS, 3, 8, HID),
        bias,
        shrink.transpose(0, 2, 1).reshape(LAYERS, 3, 8, HID),
        *tables,
    )


def solution(mesh):
    placed = (
        P("rows", "chan", None),
        P(None, None, "chan", None),
        P(None, "chan"),
        P(None, "chan"),
        P(None, "rows", "chan"),
        P(None, "chan"),
        P(None, "chan", "rows"),
    )
    return jax.shard_map(
        per_device, mesh=mesh, in_specs=placed, out_specs=P("rows", "chan", None), check_vma=False
    )
```
